512 devices in a mesh: dom: 512 (over z, y, x, core).
Axes of the slice: x: 4, y: 4, z: 16, core: 2. Of those that a mesh axis runs over, the one named last changes fastest.
Arguments:
- tracer: float32 [40, 524288], P(None, 'dom'), may hold values from -6 to 6
- bottom_levels: int32 [524288], P('dom'), may hold values from 1 to 40
- neighbours: int32 [6, 524288], P(None, 'dom'), may hold values from 0 to 2048, as said below
- edge_weight: float32 [6, 524288], P(None, 'dom'), may hold values from 0.05 to 0.5
- ssh: float32 [524288], P('dom'), may hold values from -6 to 6
- velocity: float32 [524288], P('dom'), may hold values from -3 to 3
- send_blocks: int32 [512, 4, 2], P('dom'), may hold values from -1 to 7
- thickness: float32 [40], replicated, may hold values from 0.5 to 4
- profile: float32 [40], replicated, may hold values from -4 to 4
Outputs:
- tracer_out: float32 [40, 524288], P(None, 'dom')
- ssh_out: float32 [524288], P('dom')
- velocity_out: float32 [524288], P('dom')
The draws below stay inside these ranges and needn't reach their ends.
Inputs may be any that keep to these rules, and one draw needn't show every extreme that they name: `neighbours`: entries 0 to 1023 are the partition's own cells, the next 1024 its received halo cells in the order of ext, and 2048 is land. `send_blocks`: -1 marks an empty slot; other entries are block numbers within the sending partition.
All inputs are finite; a program needn't handle non-finite values.
Results may differ from the reference program's by a relative error of at most 0.0003.
Values sent between devices are 32-bit elements; how exact they have to be, the bound alone decides.
A program may use at most 64 MiB of HBM per device.

```python
import math
import jax
import jax.numpy as jnp

BLOCK = 128
BLK_DEV = 8
LEV = 40
SEND = 2
SUBSTEPS = 6
CELLS_DEV = 1024
HALO = 1024
TOTAL_CELLS = 524288
N_DOM = 512


def draw_neighbours(key, part):
    first_key, second_key, third_key = jax.random.split(jax.random.fold_in(key, 11), 3)
    shape = (6, TOTAL_CELLS)
    kinds = jax.random.randint(first_key, shape, 0, 20)
    position = jnp.arange(TOTAL_CELLS, dtype=jnp.int32)[None, :] % CELLS_DEV
    nearby = jnp.clip(position + jax.random.randint(second_key, shape, -256, 257), 0, CELLS_DEV - 1)
    remote = CELLS_DEV + jax.random.randint(third_key, shape, 0, HALO)
    landed = jnp.full(shape, CELLS_DEV + HALO, jnp.int32)
    return jnp.where(kinds == 0, landed, jnp.where(kinds <= 4, remote, nearby)).astype(jnp.int32)


def touch_ends(array, stream_key, smallest, largest):
    extent = array.shape
    index_at = [jax.random.randint(jax.random.fold_in(stream_key, axis), (), 0, extent[axis]) for axis in range(len(extent))]
    array = array.at[tuple(index_at)].set(smallest)
    longest = extent.index(max(extent))
    index_at[longest] = (index_at[longest] + 1) % extent[longest]
    return array.at[tuple(index_at)].set(largest)


def shard_levels(own_key, dims, cuts, smallest, largest):
    factor_of, own = 1.0, jax.random.fold_in(own_key, 6)
    for dim, shards_of in cuts:
        steps = jnp.exp(jax.random.uniform(jax.random.fold_in(own, dim), (shards_of,), jnp.float32, smallest / len(cuts), largest / len(cuts)))
        factor_of = factor_of * jnp.repeat(steps, dims[dim] // shards_of).reshape([-1 if axis == dim else 1 for axis in range(len(dims))])
    return factor_of


def gaussian(key, dims, deviation, limit, cuts=(), kind=jnp.bfloat16):
    drawn = deviation * jax.random.normal(key, dims, jnp.float32)
    if cuts:
        drawn = drawn * shard_levels(key, dims, cuts, -0.22, 0.18)
    return jnp.clip(drawn, -limit, limit).astype(kind)


def setup_inputs(seed: int = 0) -> dict:
    key_of = jax.random.split(jax.random.key(seed), 10)
    tracer = gaussian(key_of[0], (LEV, TOTAL_CELLS), 1.0, 6.0, ((1, 512),), jnp.float32)
    bottom_levels = touch_ends(jax.random.randint(key_of[1], (TOTAL_CELLS,), 1, LEV + 1), jax.random.fold_in(key_of[1], 1), 1, LEV).astype(jnp.int32)
    neighbours = draw_neighbours(jax.random.fold_in(key_of[9], 71), 0)
    edge_weight = jnp.clip(jnp.exp(math.log(0.5) - 2.3025851 * jax.random.uniform(key_of[3], (6, TOTAL_CELLS), jnp.float32) ** shard_levels(key_of[3], (6, TOTAL_CELLS), ((1, 512),), -0.2, 0.2)), 0.05, 0.5)
    ssh = gaussian(key_of[4], (TOTAL_CELLS,), 1.0, 6.0, ((0, 512),), jnp.float32)
    velocity = gaussian(key_of[5], (TOTAL_CELLS,), 0.5, 3.0, ((0, 512),), jnp.float32)
    send_blocks = touch_ends(jax.random.randint(key_of[6], (N_DOM, 4, SEND), -1, BLK_DEV), jax.random.fold_in(key_of[6], 1), -1, BLK_DEV - 1).astype(jnp.int32)
    thickness = jnp.clip(jnp.exp(jax.random.uniform(key_of[7], (LEV,), jnp.float32, math.log(0.5), math.log(4.0))), 0.5, 4.0)
    profile = gaussian(key_of[8], (LEV,), 1.0, 4.0, (), jnp.float32)
    return {"tracer": tracer, "bottom_levels": bottom_levels, "neighbours": neighbours, "edge_weight": edge_weight, "ssh": ssh, "velocity": velocity, "send_blocks": send_blocks, "thickness": thickness, "profile": profile}


OFFSETS = (1, -1, 2, -2)
horizontal_rate = 0.5
vertical_rate = 0.5
tracer_step = 0.2
barotropic_step = 0.5
friction = 0.05


def extend(field, send_blocks):
    cells = BLK_DEV * BLOCK
    leading = field.shape[:-1]
    blocks = field.reshape(leading + (N_DOM * BLK_DEV, BLOCK))
    owners = jnp.arange(N_DOM, dtype=jnp.int32)
    pieces = [field.reshape(leading + (N_DOM, cells))]
    for number in range(4):
        source = owners - OFFSETS[number]
        inside = (source >= 0) & (source < N_DOM)
        clipped = jnp.clip(source, 0, N_DOM - 1).astype(jnp.int32)
        chosen = send_blocks[clipped, number]
        living = (inside[:, None] & (chosen >= 0)).astype(field.dtype)
        global_index = (clipped[:, None] * BLK_DEV + jnp.maximum(chosen, 0)).astype(jnp.int32)
        taken = jnp.take(blocks, global_index.reshape(-1), axis=-2)
        taken = taken.reshape(leading + (N_DOM, SEND * BLOCK))
        pieces.append(taken * jnp.repeat(living, BLOCK, axis=1))
    pieces.append(jnp.zeros(leading + (N_DOM, BLOCK), field.dtype))
    return jnp.concatenate(pieces, axis=-1)


def reference(tracer, bottom_levels, neighbours, edge_weight, ssh, velocity, send_blocks, thickness, profile):
    cells = BLK_DEV * BLOCK
    levels_f = bottom_levels.astype(jnp.float32)
    ext_tracer = extend(tracer, send_blocks)
    ext_levels = extend(levels_f, send_blocks)
    own_tracer = tracer.reshape(LEV, N_DOM, cells)
    own_levels = levels_f.reshape(N_DOM, cells)
    level_index = jnp.arange(LEV).astype(jnp.float32)[:, None, None]
    active = (level_index < own_levels[None]).astype(jnp.float32)
    tables = neighbours.reshape(6, N_DOM, cells)
    weights = edge_weight.reshape(6, N_DOM, cells)
    horizontal = jnp.zeros_like(own_tracer)
    for column in range(6):
        index = tables[column]
        near_levels = jnp.take_along_axis(ext_levels, index, axis=-1)
        near_active = (level_index < near_levels[None]).astype(jnp.float32)
        wide_index = jnp.broadcast_to(index[None], (LEV, N_DOM, cells))
        near_tracer = jnp.take_along_axis(ext_tracer, wide_index, axis=-1)
        horizontal = horizontal + weights[column][None] * near_active * (near_tracer - own_tracer)
    horizontal = horizontal * active
    zero_level = jnp.zeros((1, N_DOM, cells), own_tracer.dtype)
    below = jnp.concatenate([active[1:] * (own_tracer[1:] - own_tracer[:-1]), zero_level], axis=0)
    above = jnp.concatenate([zero_level, active[:-1] * (own_tracer[:-1] - own_tracer[1:])], axis=0)
    vertical = active * (below + above)
    tendency = horizontal_rate * horizontal + vertical_rate * vertical
    layers = active * thickness[:, None, None]
    forcing = jnp.sum(layers * own_tracer, axis=0) / jnp.sum(layers, axis=0)
    height = ssh.reshape(N_DOM, cells)
    speed = velocity.reshape(N_DOM, cells)
    summed = jnp.zeros_like(speed)
    for counter in range(SUBSTEPS):
        extended = extend(height.reshape(-1), send_blocks)
        laplace = jnp.zeros_like(height)
        for column in range(6):
            near_height = jnp.take_along_axis(extended, tables[column], axis=-1)
            laplace = laplace + weights[column] * (near_height - height)
        speed = (1.0 - friction) * speed + barotropic_step * (laplace + forcing)
        height = height + barotropic_step * speed
        summed = summed + speed
    tracer_out = own_tracer + tracer_step * tendency + active * profile[:, None, None] * (summed / SUBSTEPS)[None]
    return tracer_out.reshape(LEV, N_DOM * cells), height.reshape(-1), speed.reshape(-1)
```

```python
import functools

import jax
import jax.numpy as jnp
from jax import lax
from jax.experimental import pallas as pl
from jax.experimental.pallas import tpu as pltpu
from jax.sharding import PartitionSpec as P

BLOCK = 128
ROWS = 8
LEV = 40
GROUPS = LEV // 8
SUBSTEPS = 6
OFFSETS = (1, -1, 2, -2)
horizontal_rate = 0.5
vertical_rate = 0.5
tracer_step = 0.2
barotropic_step = 0.5
friction = 0.05


def along(values, index, axis):
    return jnp.take_along_axis(values, index, axis=axis, mode="promise_in_bounds")


def cols(block):
    return pl.ds(block * BLOCK, BLOCK)


def kernel(
    parts, tracer_hbm, bottom_hbm, near_hbm, weight_hbm, ssh_hbm, velocity_hbm, slots, thickness, profile,
    tracer_out, ssh_out, velocity_out,
    tracer_v, bottom_v, near_v, weight_v, ssh_v, velocity_v, result_v,
    send_tracer, halo_tracer, send_level, halo_level, send_height, halo_height,
    near_row, near_lane, weight_s, near_level, forcing_v, summed_v,
    copy_sem, tracer_send, tracer_recv, level_send, level_recv, height_send, height_recv, out_sem,
):
    me = lax.axis_index("dom")

    def start(source, target, number):
        copy = pltpu.make_async_copy(source, target, copy_sem.at[number])
        copy.start()
        return copy

    ssh_copy = start(ssh_hbm, ssh_v, 0)
    bottom_copy = start(bottom_hbm, bottom_v, 1)
    near_copy = start(near_hbm, near_v, 2)
    weight_copy = start(weight_hbm, weight_v, 3)
    tracer_copy = start(tracer_hbm, tracer_v, 4)
    velocity_copy = start(velocity_hbm, velocity_v, 5)

    def to_exists(number):
        target = me + OFFSETS[number]
        return (target >= 0) & (target < parts)

    def from_exists(number):
        source = me - OFFSETS[number]
        return (source >= 0) & (source < parts)

    barrier = pltpu.get_barrier_semaphore()
    for number in range(4):
        @pl.when(to_exists(number))
        def _(number=number):
            pl.semaphore_signal(barrier, inc=1, device_id=(me + OFFSETS[number],), device_id_type=pl.DeviceIdType.MESH)

    row_id = lax.broadcasted_iota(jnp.int32, (ROWS, BLOCK), 0)
    zero = jnp.zeros((ROWS, BLOCK), jnp.float32)
    chosen = zero.astype(jnp.int32)
    for number in range(4):
        for slot in range(2):
            chosen = jnp.where(row_id == 2 * number + slot, slots[0, slot, number], chosen)
    living = jnp.where(chosen >= 0, 1.0, 0.0)
    picked = jnp.maximum(chosen, 0)
    for number in range(4):
        @pl.when(jnp.logical_not(from_exists(number)))
        def _(number=number):
            halo_level[number] = jnp.zeros((2, BLOCK), jnp.float32)
            halo_tracer[number] = jnp.zeros((2, LEV, BLOCK), jnp.float32)
            for step in range(SUBSTEPS):
                halo_height[step, number] = jnp.zeros((2, BLOCK), jnp.float32)

    ssh_copy.wait()
    bottom_copy.wait()
    height = ssh_v[...]
    levels = bottom_v[...].astype(jnp.float32)
    sent = along(levels, picked, 0) * living
    first = along(height, picked, 0) * living
    for number in range(4):
        send_height[0, number] = first[2 * number:2 * number + 2]
        send_level[number] = sent[2 * number:2 * number + 2]

    def height_copy(step, number):
        return pltpu.make_async_remote_copy(
            src_ref=send_height.at[step, number], dst_ref=halo_height.at[step, number],
            send_sem=height_send.at[step, number], recv_sem=height_recv.at[step, number],
            device_id=(me + OFFSETS[number],), device_id_type=pl.DeviceIdType.MESH)

    def level_copy(number):
        return pltpu.make_async_remote_copy(
            src_ref=send_level.at[number], dst_ref=halo_level.at[number],
            send_sem=level_send.at[number], recv_sem=level_recv.at[number],
            device_id=(me + OFFSETS[number],), device_id_type=pl.DeviceIdType.MESH)

    def field_copy(number):
        return pltpu.make_async_remote_copy(
            src_ref=send_tracer.at[number], dst_ref=halo_tracer.at[number],
            send_sem=tracer_send.at[number], recv_sem=tracer_recv.at[number],
            device_id=(me + OFFSETS[number],), device_id_type=pl.DeviceIdType.MESH)

    def when_sending(action):
        for number in range(4):
            @pl.when(to_exists(number))
            def _(number=number):
                action(number)

    def when_receiving(action):
        for number in range(4):
            @pl.when(from_exists(number))
            def _(number=number):
                action(number)

    pl.semaphore_wait(barrier, sum(to_exists(number).astype(jnp.int32) for number in range(4)))
    when_sending(lambda number: height_copy(0, number).start())
    when_sending(lambda number: level_copy(number).start())

    tracer_copy.wait()
    for place in range(ROWS):
        which = jnp.broadcast_to(chosen[place:place + 1], (8, BLOCK))
        for group in range(GROUPS):
            piece = zero
            for block in range(ROWS):
                piece = jnp.where(which == block, tracer_v[pl.ds(group * 8, 8), cols(block)], piece)
            send_tracer[place // 2, place % 2, pl.ds(group * 8, 8), :] = piece
    when_sending(lambda number: field_copy(number).start())

    near_copy.wait()
    weight_copy.wait()
    total_weight = zero
    for column in range(6):
        for block in range(ROWS):
            near_row[column, block:block + 1] = near_v[column:column + 1, cols(block)]
            weight_s[column, block:block + 1] = weight_v[column:column + 1, cols(block)]
    for column in range(6):
        index = near_row[column]
        near_lane[column] = index & (BLOCK - 1)
        near_row[column] = index >> 7
        total_weight = total_weight + weight_s[column]

    def gather_rows(rows, first_row, sums):
        sums = list(sums)
        spread = [jnp.broadcast_to(rows[r:r + 1], (ROWS, BLOCK)) for r in range(ROWS)]
        for column in range(6):
            lane = near_lane[column]
            row = near_row[column]
            for r in range(ROWS):
                sums[column] = jnp.where(row == first_row + r, along(spread[r], lane, 1), sums[column])
        return sums

    def halo_rows(ref, *lead):
        return jnp.concatenate([ref[(*lead, number)] for number in range(4)], axis=0)

    level_id = lax.broadcasted_iota(jnp.int32, (8, BLOCK), 0)
    thick, shape = [], []
    for group in range(GROUPS):
        t, p = zero, zero
        for k in range(8):
            t = jnp.where(level_id == k, thickness[group * 8 + k], t)
            p = jnp.where(level_id == k, profile[group * 8 + k], p)
        thick.append(t)
        shape.append(p)
    level_f = level_id.astype(jnp.float32)
    for block in range(ROWS):
        own = jnp.broadcast_to(levels[block:block + 1], (8, BLOCK))
        top, bottom = zero, zero
        for group in range(GROUPS):
            layer = jnp.where(level_f + float(group * 8) < own, thick[group], 0.0)
            top = top + layer * tracer_v[pl.ds(group * 8, 8), cols(block)]
            bottom = bottom + layer
        forcing_v[block:block + 1] = jnp.sum(top, axis=0, keepdims=True) / jnp.sum(bottom, axis=0, keepdims=True)
    forcing = forcing_v[...]
    velocity_copy.wait()
    speed = velocity_v[...]

    def tracer_block(block, carry):
        at = pl.ds(pl.multiple_of(block * BLOCK, BLOCK), BLOCK)
        fields = [tracer_v[pl.ds(group * 8, 8), at] for group in range(GROUPS)]
        own = jnp.broadcast_to(bottom_v[pl.ds(block, 1), :].astype(jnp.float32), (8, BLOCK))
        sums = [zero] * GROUPS
        for column in range(6):
            index = jnp.broadcast_to(near_v[column:column + 1, at], (8, BLOCK))
            weight = jnp.broadcast_to(weight_v[column:column + 1, at], (8, BLOCK))
            depth = jnp.broadcast_to(near_level[column, pl.ds(block, 1), :], (8, BLOCK))
            lane = index & (BLOCK - 1)
            row = index >> 7
            got = [zero] * GROUPS
            for r in range(2 * ROWS):
                here = row == r
                for group in range(GROUPS):
                    if r < ROWS:
                        table = tracer_v[pl.ds(group * 8, 8), cols(r)]
                    else:
                        table = halo_tracer[(r - ROWS) // 2, (r - ROWS) % 2, pl.ds(group * 8, 8), :]
                    got[group] = jnp.where(here, along(table, lane, 1), got[group])
            for group in range(GROUPS):
                wet = jnp.where(level_f + float(group * 8) < depth, weight, 0.0)
                sums[group] = sums[group] + wet * (got[group] - fields[group])
        for group in range(GROUPS):
            here = fields[group]
            k = level_f + float(group * 8)
            down = jnp.concatenate([here[1:], fields[group + 1][:1] if group < GROUPS - 1 else here[7:]], axis=0)
            up = jnp.concatenate([fields[group - 1][7:] if group else here[:1], here[:7]], axis=0)
            vertical = jnp.where(k + 1.0 < own, down - here, 0.0) + (up - here)
            tendency = horizontal_rate * sums[group] + vertical_rate * vertical
            result_v[pl.ds(group * 8, 8), at] = here + jnp.where(k < own, tracer_step * tendency, 0.0)
        return carry

    summed = zero
    for step in range(SUBSTEPS):
        if step == 1:
            when_receiving(lambda number: field_copy(number).wait_recv())
        if 1 <= step <= 4:
            lax.fori_loop(2 * (step - 1), 2 * step, tracer_block, 0)
        sums = gather_rows(height, 0, [zero] * 6)
        when_receiving(lambda number: height_copy(step, number).wait_recv())
        sums = gather_rows(halo_rows(halo_height, step), ROWS, sums)
        laplace = -total_weight * height
        for column in range(6):
            laplace = laplace + weight_s[column] * sums[column]
        speed = (1.0 - friction) * speed + barotropic_step * (laplace + forcing)
        height = height + barotropic_step * speed
        summed = summed + speed
        if step < SUBSTEPS - 1:
            following = along(height, picked, 0) * living
            for number in range(4):
                send_height[step + 1, number] = following[2 * number:2 * number + 2]
            when_sending(lambda number: height_copy(step + 1, number).start())
        if step == 0:
            when_receiving(lambda number: level_copy(number).wait_recv())
            depths = gather_rows(levels, 0, [zero] * 6)
            depths = gather_rows(halo_rows(halo_level), ROWS, depths)
            for column in range(6):
                near_level[column] = depths[column]

    ssh_v[...] = height
    velocity_v[...] = speed
    ssh_back = pltpu.make_async_copy(ssh_v, ssh_out, out_sem.at[0])
    velocity_back = pltpu.make_async_copy(velocity_v, velocity_out, out_sem.at[1])
    ssh_back.start()
    velocity_back.start()
    mean = summed * (1.0 / SUBSTEPS)
    for block in range(ROWS):
        own = jnp.broadcast_to(levels[block:block + 1], (8, BLOCK))
        push = jnp.broadcast_to(mean[block:block + 1], (8, BLOCK))
        for group in range(GROUPS):
            at = (pl.ds(group * 8, 8), cols(block))
            result_v[at] = result_v[at] + jnp.where(level_f + float(group * 8) < own, shape[group] * push, 0.0)
    back = pltpu.make_async_copy(result_v, tracer_out, out_sem.at[2])
    back.start()
    for step in range(SUBSTEPS):
        when_sending(lambda number: height_copy(step, number).wait_send())
    when_sending(lambda number: level_copy(number).wait_send())
    when_sending(lambda number: field_copy(number).wait_send())
    ssh_back.wait()
    velocity_back.wait()
    back.wait()


def solution(mesh):
    parts = mesh.shape["dom"]

    def shards(tracer, bottom, near, weight, ssh, velocity, slots, thickness, profile):
        hbm = pl.BlockSpec(memory_space=pltpu.HBM)
        smem = pl.BlockSpec(memory_space=pltpu.SMEM)
        tile = (ROWS, BLOCK)
        f32 = jnp.float32
        wide = (LEV, ROWS * BLOCK)
        out = pl.pallas_call(
            functools.partial(kernel, parts),
            out_shape=(jax.ShapeDtypeStruct(wide, f32), jax.ShapeDtypeStruct(tile, f32), jax.ShapeDtypeStruct(tile, f32)),
            in_specs=[hbm] * 6 + [smem] * 3,
            out_specs=(hbm, hbm, hbm),
            scratch_shapes=[
                pltpu.VMEM(wide, f32), pltpu.VMEM(tile, jnp.int32), pltpu.VMEM((6, ROWS * BLOCK), jnp.int32),
                pltpu.VMEM((6, ROWS * BLOCK), f32), pltpu.VMEM(tile, f32), pltpu.VMEM(tile, f32), pltpu.VMEM(wide, f32),
                pltpu.VMEM((4, 2, LEV, BLOCK), f32), pltpu.VMEM((4, 2, LEV, BLOCK), f32),
                pltpu.VMEM((4, 2, BLOCK), f32), pltpu.VMEM((4, 2, BLOCK), f32),
                pltpu.VMEM((SUBSTEPS, 4, 2, BLOCK), f32), pltpu.VMEM((SUBSTEPS, 4, 2, BLOCK), f32),
                pltpu.VMEM((6, *tile), jnp.int32), pltpu.VMEM((6, *tile), jnp.int32), pltpu.VMEM((6, *tile), f32),
                pltpu.VMEM((6, *tile), f32), pltpu.VMEM(tile, f32), pltpu.VMEM(tile, f32),
                pltpu.SemaphoreType.DMA((6,)),
                pltpu.SemaphoreType.DMA((4,)), pltpu.SemaphoreType.DMA((4,)),
                pltpu.SemaphoreType.DMA((4,)), pltpu.SemaphoreType.DMA((4,)),
                pltpu.SemaphoreType.DMA((SUBSTEPS, 4)), pltpu.SemaphoreType.DMA((SUBSTEPS, 4)),
                pltpu.SemaphoreType.DMA((3,)),
            ],
            compiler_params=pltpu.CompilerParams(collective_id=0, has_side_effects=True),
        )(tracer, bottom.reshape(tile), near, weight, ssh.reshape(tile), velocity.reshape(tile), jnp.transpose(slots, (0, 2, 1)), thickness, profile)
        return out[0], out[1].reshape(-1), out[2].reshape(-1)

    placed = (P(None, "dom"), P("dom"), P(None, "dom"), P(None, "dom"), P("dom"), P("dom"), P("dom", None, None), P(), P())
    return jax.shard_map(shards, mesh=mesh, in_specs=placed, out_specs=(P(None, "dom"), P("dom"), P("dom")), check_vma=False)
```

```python
import functools

import jax
import jax.numpy as jnp
from jax import lax
from jax.experimental import pallas as pl
from jax.experimental.pallas import tpu as pltpu
from jax.sharding import PartitionSpec as P

BLOCK = 128
ROWS = 8
LEV = 40
GROUPS = LEV // 8
SUBSTEPS = 6
OFFSETS = (1, -1, 2, -2)
horizontal_rate = 0.5
vertical_rate = 0.5
tracer_step = 0.2
barotropic_step = 0.5
friction = 0.05


FAR = (3, -3, 4, -4)
PLACE = (0, 2, 1, 3)
FAR_ROWS = ((0, 2), (2, 4), (1, 2), (3, 4))
ROUNDS = SUBSTEPS // 2
LAND = 2 * ROWS * BLOCK
TILE = (ROWS, BLOCK)


def along(values, index, axis):
    return jnp.take_along_axis(values, index, axis=axis, mode="promise_in_bounds")


def cols(block):
    return pl.ds(block * BLOCK, BLOCK)


def spread(row):
    return jnp.broadcast_to(row, TILE)


def kernel(
    parts, tracer_hbm, bottom_hbm, near_hbm, weight_hbm, ssh_hbm, velocity_hbm, slots, thickness,
    base_out, tail_out,
    tracer_v, bottom_v, near_v, weight_v, ssh_v, velocity_v, base_v, tail_v,
    send_tracer, halo_tracer, send_level, halo_level, send_chosen, halo_chosen,
    send_near, halo_near, send_weight, halo_weight,
    send_height, halo_height, send_picked, halo_three, halo_four, send_push, halo_push,
    near_row, near_lane, weight_s, near_level, forcing_v,
    copy_sem, out_sem, tracer_sem, level_sem, chosen_sem, near_sem, weight_sem, height_sem, far_sem, push_sem,
):
    me = lax.axis_index("dom")

    def start(source, target, number):
        copy = pltpu.make_async_copy(source, target, copy_sem.at[number])
        copy.start()
        return copy

    tracer_copy = start(tracer_hbm, tracer_v, 4)
    bottom_copy = start(bottom_hbm, bottom_v, 1)
    near_copy = start(near_hbm, near_v, 2)
    weight_copy = start(weight_hbm, weight_v, 3)
    ssh_copy = start(ssh_hbm, ssh_v, 0)
    velocity_copy = start(velocity_hbm, velocity_v, 5)

    def inside(place):
        return (place >= 0) & (place < parts)

    barrier = pltpu.get_barrier_semaphore()
    for offset in OFFSETS + FAR:
        @pl.when(inside(me + offset))
        def _(offset=offset):
            pl.semaphore_signal(barrier, inc=1, device_id=(me + offset,), device_id_type=pl.DeviceIdType.MESH)

    row_id = lax.broadcasted_iota(jnp.int32, TILE, 0)
    level_f = row_id.astype(jnp.float32)
    zero = jnp.zeros(TILE, jnp.float32)

    for number in range(4):
        @pl.when(jnp.logical_not(inside(me - OFFSETS[number])))
        def _(number=number):
            halo_chosen[number] = jnp.full(TILE, -1, jnp.int32)
            halo_near[number] = jnp.full((2, *TILE), LAND, jnp.int32)
            halo_weight[number] = jnp.zeros((2, *TILE), jnp.float32)
            halo_level[number] = jnp.zeros((2, BLOCK), jnp.float32)
            halo_tracer[number] = jnp.zeros((2, LEV, BLOCK), jnp.float32)
            for turn in range(ROUNDS):
                halo_height[turn, number] = zero
                halo_push[turn, number] = jnp.zeros((2, BLOCK), jnp.float32)
        @pl.when(jnp.logical_not(inside(me - FAR[number])))
        def _(number=number):
            for turn in range(ROUNDS):
                if number < 2:
                    halo_three[turn, number] = jnp.zeros((2, 2, BLOCK), jnp.float32)
                else:
                    halo_four[turn, number - 2] = jnp.zeros((1, 2, BLOCK), jnp.float32)

    def remote(source, target, sems, offset):
        return pltpu.make_async_remote_copy(
            src_ref=source, dst_ref=target, send_sem=sems.at[0], recv_sem=sems.at[1],
            device_id=(me + offset,), device_id_type=pl.DeviceIdType.MESH)

    def tracer_link(n):
        return remote(send_tracer.at[n], halo_tracer.at[n], tracer_sem.at[n], OFFSETS[n])

    def level_link(n):
        return remote(send_level.at[n], halo_level.at[n], level_sem.at[n], OFFSETS[n])

    def chosen_link(n):
        return remote(send_chosen, halo_chosen.at[n], chosen_sem.at[n], OFFSETS[n])

    def near_link(n):
        return remote(send_near.at[n], halo_near.at[n], near_sem.at[n], OFFSETS[n])

    def weight_link(n):
        return remote(send_weight.at[n], halo_weight.at[n], weight_sem.at[n], OFFSETS[n])

    def height_link(turn, n):
        return remote(send_height.at[turn], halo_height.at[turn, n], height_sem.at[turn, n], OFFSETS[n])

    def push_link(turn, n):
        return remote(send_push.at[turn, n], halo_push.at[turn, n], push_sem.at[turn, n], OFFSETS[n])

    def far_link(turn, n):
        low, high = FAR_ROWS[n]
        target = halo_three.at[turn, n] if n < 2 else halo_four.at[turn, n - 2]
        return remote(send_picked.at[turn, pl.ds(low, high - low)], target, far_sem.at[turn, n], FAR[n])

    def begin(links, offsets=OFFSETS):
        for number in range(4):
            @pl.when(inside(me + offsets[number]))
            def _(number=number):
                for link in links:
                    link(number).start()

    def arrive(links, offsets=OFFSETS):
        for number in range(4):
            @pl.when(inside(me - offsets[number]))
            def _(number=number):
                for link in links:
                    link(number).wait_recv()

    def leave(links, offsets=OFFSETS):
        for number in range(4):
            @pl.when(inside(me + offsets[number]))
            def _(number=number):
                for link in links:
                    link(number).wait_send()

    chosen = zero.astype(jnp.int32)
    for number in range(4):
        for slot in range(2):
            chosen = jnp.where(row_id == 2 * number + slot, slots[0, slot, number], chosen)
    send_chosen[...] = chosen

    def pick(values, choice):
        return jnp.where(choice >= 0, along(values, jnp.maximum(choice, 0), 0), 0.0)

    def put_round(turn, height, push):
        picked = pick(height, chosen)
        pushed = pick(push, chosen)
        send_height[turn] = height
        for number in range(4):
            send_picked[turn, PLACE[number]] = picked[2 * number:2 * number + 2]
            send_push[turn, number] = pushed[2 * number:2 * number + 2]
        return picked

    bottom_copy.wait()
    levels = bottom_v[...].astype(jnp.float32)
    sent_levels = pick(levels, chosen)
    for number in range(4):
        send_level[number] = sent_levels[2 * number:2 * number + 2]
    thick = []
    for group in range(GROUPS):
        t = zero
        for k in range(8):
            t = jnp.where(row_id == k, thickness[group * 8 + k], t)
        thick.append(t)
    tracer_copy.wait()
    for block in range(ROWS):
        own = spread(levels[block:block + 1])
        top, under = zero, zero
        for group in range(GROUPS):
            layer = jnp.where(level_f + float(group * 8) < own, thick[group], 0.0)
            top = top + layer * tracer_v[pl.ds(group * 8, 8), cols(block)]
            under = under + layer
        forcing_v[block:block + 1] = jnp.sum(top, axis=0, keepdims=True) / jnp.sum(under, axis=0, keepdims=True)
    forcing = forcing_v[...]
    ssh_copy.wait()
    velocity_copy.wait()
    height = ssh_v[...]

    def pushed_by(speed):
        return (1.0 - friction) * speed + barotropic_step * forcing

    push = pushed_by(velocity_v[...])
    picked = put_round(0, height, push)

    near_copy.wait()
    weight_copy.wait()
    for place in range(ROWS):
        which = spread(chosen[place:place + 1])
        n, slot = place // 2, place % 2
        index = jnp.full((6, BLOCK), LAND, jnp.int32)
        amount = jnp.zeros((6, BLOCK), jnp.float32)
        for block in range(ROWS):
            index = jnp.where(which[:6] == block, near_v[:, cols(block)], index)
            amount = jnp.where(which[:6] == block, weight_v[:, cols(block)], amount)
        send_near[n, slot] = jnp.full(TILE, LAND, jnp.int32)
        send_weight[n, slot] = zero
        send_near[n, slot, 0:6] = index
        send_weight[n, slot, 0:6] = amount
    total_weight = zero
    for column in range(6):
        for block in range(ROWS):
            near_row[column, block:block + 1] = near_v[column:column + 1, cols(block)]
            weight_s[column, block:block + 1] = weight_v[column:column + 1, cols(block)]
    for column in range(6):
        index = near_row[column]
        near_lane[column] = index & (BLOCK - 1)
        near_row[column] = index >> 7
        total_weight = total_weight + weight_s[column]
    for place in range(ROWS):
        which = spread(chosen[place:place + 1])
        for group in range(GROUPS):
            piece = zero
            for block in range(ROWS):
                piece = jnp.where(which == block, tracer_v[pl.ds(group * 8, 8), cols(block)], piece)
            send_tracer[place // 2, place % 2, pl.ds(group * 8, 8), :] = piece

    pl.semaphore_wait(barrier, sum(inside(me + offset).astype(jnp.int32) for offset in OFFSETS + FAR))
    begin([functools.partial(far_link, 0)], FAR)
    begin([functools.partial(height_link, 0), chosen_link, near_link, weight_link, functools.partial(push_link, 0)])
    begin([level_link, tracer_link])

    def gather(rows, first_row, columns, sums):
        sums = list(sums)
        wide = [spread(rows[r:r + 1]) for r in range(ROWS)]
        for i, (row, lane) in enumerate(columns):
            for r in range(ROWS):
                sums[i] = jnp.where(row == first_row + r, along(wide[r], lane, 1), sums[i])
        return sums

    def own_columns():
        return [(near_row[column], near_lane[column]) for column in range(6)]

    def own_update(sums, height, push):
        laplace = -total_weight * height
        for column in range(6):
            laplace = laplace + weight_s[column] * sums[column]
        speed = push + barotropic_step * laplace
        return speed, height + barotropic_step * speed

    def tracer_block(block, carry):
        at = pl.ds(pl.multiple_of(block * BLOCK, BLOCK), BLOCK)
        fields = [tracer_v[pl.ds(group * 8, 8), at] for group in range(GROUPS)]
        own = spread(bottom_v[pl.ds(block, 1), :].astype(jnp.float32))
        sums = [zero] * GROUPS
        for column in range(6):
            index = spread(near_v[column:column + 1, at])
            weight = spread(weight_v[column:column + 1, at])
            depth = spread(near_level[column, pl.ds(block, 1), :])
            lane = index & (BLOCK - 1)
            row = index >> 7
            got = [zero] * GROUPS
            for r in range(2 * ROWS):
                here = row == r
                for group in range(GROUPS):
                    if r < ROWS:
                        table = tracer_v[pl.ds(group * 8, 8), cols(r)]
                    else:
                        table = halo_tracer[(r - ROWS) // 2, (r - ROWS) % 2, pl.ds(group * 8, 8), :]
                    got[group] = jnp.where(here, along(table, lane, 1), got[group])
            for group in range(GROUPS):
                wet = jnp.where(level_f + float(group * 8) < depth, weight, 0.0)
                sums[group] = sums[group] + wet * (got[group] - fields[group])
        for group in range(GROUPS):
            here = fields[group]
            k = level_f + float(group * 8)
            down = jnp.concatenate([here[1:], fields[group + 1][:1] if group < GROUPS - 1 else here[7:]], axis=0)
            up = jnp.concatenate([fields[group - 1][7:] if group else here[:1], here[:7]], axis=0)
            vertical = jnp.where(k + 1.0 < own, down - here, 0.0) + (up - here)
            tendency = horizontal_rate * sums[group] + vertical_rate * vertical
            base_v[pl.ds(group * 8, 8), at] = here + jnp.where(k < own, tracer_step * tendency, 0.0)
        return carry

    base_copy = pltpu.make_async_copy(base_v, base_out, out_sem.at[0])
    summed = zero
    for turn in range(ROUNDS):
        if turn == 1:
            arrive([tracer_link])
        if turn >= 1:
            lax.fori_loop(4 * (turn - 1), 4 * turn, tracer_block, 0)
        if turn == ROUNDS - 1:
            base_copy.start()
        sums = gather(height, 0, own_columns(), [zero] * 6)
        if turn == 0:
            arrive([functools.partial(height_link, turn), chosen_link])
        else:
            arrive([functools.partial(height_link, turn)])
        fields = [halo_height[turn, n] for n in range(4)]
        choices = [halo_chosen[n] for n in range(4)]
        picks = [pick(fields[n], choices[n]) for n in range(4)]
        halo = jnp.concatenate([picks[n][2 * n:2 * n + 2] for n in range(4)], axis=0)
        sums = gather(halo, ROWS, own_columns(), sums)
        arrive([functools.partial(far_link, turn)], FAR)
        if turn == 0:
            arrive([near_link, weight_link])
        arrive([functools.partial(push_link, turn)])
        laplaces = []
        for h in range(4):
            rows = []
            for g in range(4):
                gap = OFFSETS[h] + OFFSETS[g]
                if gap == 0:
                    rows.append(picked[2 * g:2 * g + 2])
                elif gap in OFFSETS:
                    rows.append(picks[OFFSETS.index(gap)][2 * g:2 * g + 2])
                else:
                    f = FAR.index(gap)
                    at = PLACE[g] - FAR_ROWS[f][0]
                    rows.append(halo_three[turn, f, at] if f < 2 else halo_four[turn, f - 2, at])
            around = jnp.concatenate(rows, axis=0)
            indices = [halo_near[h, slot] for slot in range(2)]
            columns = [(index >> 7, index & (BLOCK - 1)) for index in indices]
            found = gather(fields[h], 0, columns, [zero] * 2)
            found = gather(around, ROWS, columns, found)
            for slot in range(2):
                place = 2 * h + slot
                difference = halo_weight[h, slot] * (found[slot] - spread(halo[place:place + 1]))
                laplaces.append(jnp.sum(difference, axis=0, keepdims=True))
        outer = jnp.concatenate([halo_push[turn, n] for n in range(4)], axis=0)
        outer = outer + barotropic_step * jnp.concatenate(laplaces, axis=0)
        alive = jnp.concatenate([choices[n][2 * n:2 * n + 2] for n in range(4)], axis=0)
        halo = jnp.where(alive >= 0, halo + barotropic_step * outer, 0.0)
        speed, height = own_update(sums, height, push)
        push = pushed_by(speed)
        summed = summed + speed

        sums = gather(height, 0, own_columns(), [zero] * 6)
        sums = gather(halo, ROWS, own_columns(), sums)
        speed, height = own_update(sums, height, push)
        push = pushed_by(speed)
        summed = summed + speed
        if turn < ROUNDS - 1:
            picked = put_round(turn + 1, height, push)
            begin([functools.partial(far_link, turn + 1)], FAR)
            begin([functools.partial(height_link, turn + 1), functools.partial(push_link, turn + 1)])
        if turn == 0:
            arrive([level_link])
            depths = gather(levels, 0, own_columns(), [zero] * 6)
            around = jnp.concatenate([halo_level[n] for n in range(4)], axis=0)
            depths = gather(around, ROWS, own_columns(), depths)
            for column in range(6):
                near_level[column] = depths[column]

    tail_v[0] = height
    tail_v[1] = speed
    tail_v[2] = summed * (1.0 / SUBSTEPS)
    tail_copy = pltpu.make_async_copy(tail_v, tail_out, out_sem.at[1])
    tail_copy.start()
    for turn in range(ROUNDS):
        leave([functools.partial(far_link, turn)], FAR)
        leave([functools.partial(height_link, turn), functools.partial(push_link, turn)])
    leave([chosen_link, near_link, weight_link, level_link, tracer_link])
    base_copy.wait()
    tail_copy.wait()


def finish(base_hbm, tail_hbm, bottom_hbm, profile, tracer_out, ssh_out, velocity_out, base_v, tail_v, bottom_v, in_sem, out_sem):
    copies = [
        pltpu.make_async_copy(source, target, in_sem.at[i])
        for i, (source, target) in enumerate(((tail_hbm, tail_v), (bottom_hbm, bottom_v), (base_hbm, base_v)))
    ]
    for copy in copies:
        copy.start()
    backs = [
        pltpu.make_async_copy(source, target, out_sem.at[i])
        for i, (source, target) in enumerate(((tail_v.at[0], ssh_out), (tail_v.at[1], velocity_out), (base_v, tracer_out)))
    ]
    row_id = lax.broadcasted_iota(jnp.int32, TILE, 0)
    shape = []
    for group in range(GROUPS):
        p = jnp.zeros(TILE, jnp.float32)
        for k in range(8):
            p = jnp.where(row_id == k, profile[group * 8 + k], p)
        shape.append(p)
    copies[0].wait()
    backs[0].start()
    backs[1].start()
    copies[1].wait()
    copies[2].wait()
    mean = tail_v[2]
    levels = bottom_v[...]
    for block in range(ROWS):
        own = spread(levels[block:block + 1])
        push = spread(mean[block:block + 1])
        for group in range(GROUPS):
            at = (pl.ds(group * 8, 8), cols(block))
            base_v[at] = base_v[at] + jnp.where(row_id + group * 8 < own, shape[group] * push, 0.0)
    backs[2].start()
    for back in backs:
        back.wait()


def solution(mesh):
    parts = mesh.shape["dom"]

    def shards(tracer, bottom, near, weight, ssh, velocity, slots, thickness, profile):
        hbm = pl.BlockSpec(memory_space=pltpu.HBM)
        smem = pl.BlockSpec(memory_space=pltpu.SMEM)
        f32, i32 = jnp.float32, jnp.int32
        wide = (LEV, ROWS * BLOCK)
        dma = pltpu.SemaphoreType.DMA
        vmem = pltpu.VMEM
        levels = bottom.reshape(TILE)
        base, tail = pl.pallas_call(
            functools.partial(kernel, parts),
            out_shape=(jax.ShapeDtypeStruct(wide, f32), jax.ShapeDtypeStruct((3, *TILE), f32)),
            in_specs=[hbm] * 6 + [smem] * 2,
            out_specs=(hbm, hbm),
            scratch_shapes=[
                vmem(wide, f32), vmem(TILE, i32), vmem((6, ROWS * BLOCK), i32), vmem((6, ROWS * BLOCK), f32),
                vmem(TILE, f32), vmem(TILE, f32), vmem(wide, f32), vmem((3, *TILE), f32),
                vmem((4, 2, LEV, BLOCK), f32), vmem((4, 2, LEV, BLOCK), f32),
                vmem((4, 2, BLOCK), f32), vmem((4, 2, BLOCK), f32), vmem(TILE, i32), vmem((4, *TILE), i32),
                vmem((4, 2, *TILE), i32), vmem((4, 2, *TILE), i32), vmem((4, 2, *TILE), f32), vmem((4, 2, *TILE), f32),
                vmem((ROUNDS, *TILE), f32), vmem((ROUNDS, 4, *TILE), f32),
                vmem((ROUNDS, 4, 2, BLOCK), f32), vmem((ROUNDS, 2, 2, 2, BLOCK), f32), vmem((ROUNDS, 2, 1, 2, BLOCK), f32),
                vmem((ROUNDS, 4, 2, BLOCK), f32), vmem((ROUNDS, 4, 2, BLOCK), f32),
                vmem((6, *TILE), i32), vmem((6, *TILE), i32), vmem((6, *TILE), f32), vmem((6, *TILE), f32), vmem(TILE, f32),
                dma((6,)), dma((2,)), dma((4, 2)), dma((4, 2)), dma((4, 2)), dma((4, 2)), dma((4, 2)),
                dma((ROUNDS, 4, 2)), dma((ROUNDS, 4, 2)), dma((ROUNDS, 4, 2)),
            ],
            compiler_params=pltpu.CompilerParams(collective_id=0, has_side_effects=True),
        )(tracer, levels, near, weight, ssh.reshape(TILE), velocity.reshape(TILE), jnp.transpose(slots, (0, 2, 1)), thickness)
        tile = jax.ShapeDtypeStruct(TILE, f32)
        out = pl.pallas_call(
            finish,
            out_shape=(jax.ShapeDtypeStruct(wide, f32), tile, tile),
            in_specs=[hbm] * 3 + [smem],
            out_specs=(hbm, hbm, hbm),
            scratch_shapes=[vmem(wide, f32), vmem((3, *TILE), f32), vmem(TILE, i32), dma((3,)), dma((3,))],
        )(base, tail, levels, profile)
        return out[0], out[1].reshape(-1), out[2].reshape(-1)

    placed = (P(None, "dom"), P("dom"), P(None, "dom"), P(None, "dom"), P("dom"), P("dom"), P("dom", None, None), P(), P())
    return jax.shard_map(shards, mesh=mesh, in_specs=placed, out_specs=(P(None, "dom"), P("dom"), P("dom")), check_vma=False)
```

```python
import functools

import jax
import jax.numpy as jnp
from jax import lax
from jax.experimental import pallas as pl
from jax.experimental.pallas import tpu as pltpu
from jax.sharding import PartitionSpec as P

BLOCK = 128
ROWS = 8
LEV = 40
GROUPS = LEV // 8
SUBSTEPS = 6
OFFSETS = (1, -1, 2, -2)
horizontal_rate = 0.5
vertical_rate = 0.5
tracer_step = 0.2
barotropic_step = 0.5
friction = 0.05


FAR = (3, -3, 4, -4)
PLACE = (0, 2, 1, 3)
FAR_ROWS = ((0, 2), (2, 4), (1, 2), (3, 4))
ROUNDS = SUBSTEPS // 2
LAND = 2 * ROWS * BLOCK
TILE = (ROWS, BLOCK)


def along(values, index, axis):
    return jnp.take_along_axis(values, index, axis=axis, mode="promise_in_bounds")


def cols(block):
    return pl.ds(block * BLOCK, BLOCK)


def spread(row):
    return jnp.broadcast_to(row, TILE)


def kernel(
    parts, tracer_hbm, bottom_hbm, near_hbm, weight_hbm, ssh_hbm, velocity_hbm, slots_hbm, thickness_hbm, profile_hbm,
    base_v, tail_v,
    tracer_v, bottom_v, near_v, weight_v, ssh_v, velocity_v, slots, thickness, profile,
    send_tracer, halo_tracer, send_level, halo_level, send_chosen, halo_chosen,
    send_near, halo_near, send_weight, halo_weight,
    send_height, halo_height, send_picked, halo_three, halo_four, send_push, halo_push,
    near_row, near_lane, weight_s, near_level, forcing_v,
    copy_sem, tracer_sem, level_sem, chosen_sem, near_sem, weight_sem, height_sem, far_sem, push_sem,
):
    me = lax.axis_index("dom")

    def start(source, target, number):
        copy = pltpu.make_async_copy(source, target, copy_sem.at[number])
        copy.start()
        return copy

    def inside(place):
        return (place >= 0) & (place < parts)

    barrier = pltpu.get_barrier_semaphore()
    for offset in OFFSETS + FAR:
        @pl.when(inside(me + offset))
        def _(offset=offset):
            pl.semaphore_signal(barrier, inc=1, device_id=(me + offset,), device_id_type=pl.DeviceIdType.MESH)

    slots_copy = start(slots_hbm, slots, 6)
    thickness_copy = start(thickness_hbm, thickness, 7)
    profile_copy = start(profile_hbm, profile, 8)
    tracer_copy = start(tracer_hbm, tracer_v, 4)
    bottom_copy = start(bottom_hbm, bottom_v, 1)
    near_copy = start(near_hbm, near_v, 2)
    weight_copy = start(weight_hbm, weight_v, 3)
    ssh_copy = start(ssh_hbm, ssh_v, 0)
    velocity_copy = start(velocity_hbm, velocity_v, 5)

    row_id = lax.broadcasted_iota(jnp.int32, TILE, 0)
    level_f = row_id.astype(jnp.float32)
    zero = jnp.zeros(TILE, jnp.float32)

    for number in range(4):
        @pl.when(jnp.logical_not(inside(me - OFFSETS[number])))
        def _(number=number):
            halo_chosen[number] = jnp.full(TILE, -1, jnp.int32)
            halo_near[number] = jnp.full((2, *TILE), LAND, jnp.int32)
            halo_weight[number] = jnp.zeros((2, *TILE), jnp.float32)
            halo_level[number] = jnp.zeros((2, BLOCK), jnp.float32)
            halo_tracer[number] = jnp.zeros((2, LEV, BLOCK), jnp.float32)
            for turn in range(ROUNDS):
                halo_height[turn, number] = zero
                halo_push[turn, number] = jnp.zeros((2, BLOCK), jnp.float32)
        @pl.when(jnp.logical_not(inside(me - FAR[number])))
        def _(number=number):
            for turn in range(ROUNDS):
                if number < 2:
                    halo_three[turn, number] = jnp.zeros((2, 2, BLOCK), jnp.float32)
                else:
                    halo_four[turn, number - 2] = jnp.zeros((1, 2, BLOCK), jnp.float32)

    def remote(source, target, sems, offset):
        return pltpu.make_async_remote_copy(
            src_ref=source, dst_ref=target, send_sem=sems.at[0], recv_sem=sems.at[1],
            device_id=(me + offset,), device_id_type=pl.DeviceIdType.MESH)

    def tracer_link(n):
        return remote(send_tracer.at[n], halo_tracer.at[n], tracer_sem.at[n], OFFSETS[n])

    def level_link(n):
        return remote(send_level.at[n], halo_level.at[n], level_sem.at[n], OFFSETS[n])

    def chosen_link(n):
        return remote(send_chosen, halo_chosen.at[n], chosen_sem.at[n], OFFSETS[n])

    def near_link(n):
        return remote(send_near.at[n], halo_near.at[n], near_sem.at[n], OFFSETS[n])

    def weight_link(n):
        return remote(send_weight.at[n], halo_weight.at[n], weight_sem.at[n], OFFSETS[n])

    def height_link(turn, n):
        return remote(send_height.at[turn], halo_height.at[turn, n], height_sem.at[turn, n], OFFSETS[n])

    def push_link(turn, n):
        return remote(send_push.at[turn, n], halo_push.at[turn, n], push_sem.at[turn, n], OFFSETS[n])

    def far_link(turn, n):
        low, high = FAR_ROWS[n]
        target = halo_three.at[turn, n] if n < 2 else halo_four.at[turn, n - 2]
        return remote(send_picked.at[turn, pl.ds(low, high - low)], target, far_sem.at[turn, n], FAR[n])

    def begin(links, offsets=OFFSETS):
        for number in range(4):
            @pl.when(inside(me + offsets[number]))
            def _(number=number):
                for link in links:
                    link(number).start()

    def arrive(links, offsets=OFFSETS):
        for number in range(4):
            @pl.when(inside(me - offsets[number]))
            def _(number=number):
                for link in links:
                    link(number).wait_recv()

    def leave(links, offsets=OFFSETS):
        for number in range(4):
            @pl.when(inside(me + offsets[number]))
            def _(number=number):
                for link in links:
                    link(number).wait_send()

    slots_copy.wait()
    chosen = zero.astype(jnp.int32)
    for number in range(4):
        for slot in range(2):
            chosen = jnp.where(row_id == 2 * number + slot, slots[0, slot, number], chosen)
    send_chosen[...] = chosen

    def pick(values, choice):
        return jnp.where(choice >= 0, along(values, jnp.maximum(choice, 0), 0), 0.0)

    def put_round(turn, height, push):
        picked = pick(height, chosen)
        pushed = pick(push, chosen)
        send_height[turn] = height
        for number in range(4):
            send_picked[turn, PLACE[number]] = picked[2 * number:2 * number + 2]
            send_push[turn, number] = pushed[2 * number:2 * number + 2]
        return picked

    bottom_copy.wait()
    levels = bottom_v[...].astype(jnp.float32)
    sent_levels = pick(levels, chosen)
    for number in range(4):
        send_level[number] = sent_levels[2 * number:2 * number + 2]
    thickness_copy.wait()
    profile_copy.wait()
    thick = []
    for group in range(GROUPS):
        t, p = zero, zero
        for k in range(8):
            t = jnp.where(row_id == k, thickness[group * 8 + k], t)
            p = jnp.where(row_id == k, profile[group * 8 + k], p)
        thick.append(t)
        tail_v[4 + group] = p
    tail_v[3] = levels
    tracer_copy.wait()
    for block in range(ROWS):
        own = spread(levels[block:block + 1])
        top, under = zero, zero
        for group in range(GROUPS):
            layer = jnp.where(level_f + float(group * 8) < own, thick[group], 0.0)
            top = top + layer * tracer_v[pl.ds(group * 8, 8), cols(block)]
            under = under + layer
        forcing_v[block:block + 1] = jnp.sum(top, axis=0, keepdims=True) / jnp.sum(under, axis=0, keepdims=True)
    forcing = forcing_v[...]
    ssh_copy.wait()
    velocity_copy.wait()
    height = ssh_v[...]

    def pushed_by(speed):
        return (1.0 - friction) * speed + barotropic_step * forcing

    push = pushed_by(velocity_v[...])
    picked = put_round(0, height, push)

    near_copy.wait()
    weight_copy.wait()
    for place in range(ROWS):
        which = spread(chosen[place:place + 1])
        n, slot = place // 2, place % 2
        index = jnp.full((6, BLOCK), LAND, jnp.int32)
        amount = jnp.zeros((6, BLOCK), jnp.float32)
        for block in range(ROWS):
            index = jnp.where(which[:6] == block, near_v[:, cols(block)], index)
            amount = jnp.where(which[:6] == block, weight_v[:, cols(block)], amount)
        send_near[n, slot] = jnp.full(TILE, LAND, jnp.int32)
        send_weight[n, slot] = zero
        send_near[n, slot, 0:6] = index
        send_weight[n, slot, 0:6] = amount
    total_weight = zero
    for column in range(6):
        for block in range(ROWS):
            near_row[column, block:block + 1] = near_v[column:column + 1, cols(block)]
            weight_s[column, block:block + 1] = weight_v[column:column + 1, cols(block)]
    for column in range(6):
        index = near_row[column]
        near_lane[column] = index & (BLOCK - 1)
        near_row[column] = index >> 7
        total_weight = total_weight + weight_s[column]
    for place in range(ROWS):
        which = spread(chosen[place:place + 1])
        for group in range(GROUPS):
            piece = zero
            for block in range(ROWS):
                piece = jnp.where(which == block, tracer_v[pl.ds(group * 8, 8), cols(block)], piece)
            send_tracer[place // 2, place % 2, pl.ds(group * 8, 8), :] = piece

    pl.semaphore_wait(barrier, sum(inside(me + offset).astype(jnp.int32) for offset in OFFSETS + FAR))
    begin([functools.partial(far_link, 0)], FAR)
    begin([functools.partial(height_link, 0), chosen_link, near_link, weight_link, functools.partial(push_link, 0)])
    begin([level_link, tracer_link])

    def gather(rows, first_row, columns, sums):
        sums = list(sums)
        count = rows.shape[0]
        wide = [spread(rows[r:r + 1]) for r in range(count)]
        for i, (row, lane) in enumerate(columns):
            for r in range(count):
                sums[i] = jnp.where(row == first_row + r, along(wide[r], lane, 1), sums[i])
        return sums

    def own_columns():
        return [(near_row[column], near_lane[column]) for column in range(6)]

    def own_update(sums, height, push):
        laplace = -total_weight * height
        for column in range(6):
            laplace = laplace + weight_s[column] * sums[column]
        speed = push + barotropic_step * laplace
        return speed, height + barotropic_step * speed

    def tracer_block(block, carry):
        at = pl.ds(pl.multiple_of(block * BLOCK, BLOCK), BLOCK)
        fields = [tracer_v[pl.ds(group * 8, 8), at] for group in range(GROUPS)]
        own = spread(bottom_v[pl.ds(block, 1), :].astype(jnp.float32))
        sums = [zero] * GROUPS
        for column in range(6):
            index = spread(near_v[column:column + 1, at])
            weight = spread(weight_v[column:column + 1, at])
            depth = spread(near_level[column, pl.ds(block, 1), :])
            lane = index & (BLOCK - 1)
            row = index >> 7
            got = [zero] * GROUPS
            for r in range(2 * ROWS):
                here = row == r
                for group in range(GROUPS):
                    if r < ROWS:
                        table = tracer_v[pl.ds(group * 8, 8), cols(r)]
                    else:
                        table = halo_tracer[(r - ROWS) // 2, (r - ROWS) % 2, pl.ds(group * 8, 8), :]
                    got[group] = jnp.where(here, along(table, lane, 1), got[group])
            for group in range(GROUPS):
                wet = jnp.where(level_f + float(group * 8) < depth, weight, 0.0)
                sums[group] = sums[group] + wet * (got[group] - fields[group])
        for group in range(GROUPS):
            here = fields[group]
            k = level_f + float(group * 8)
            down = jnp.concatenate([here[1:], fields[group + 1][:1] if group < GROUPS - 1 else here[7:]], axis=0)
            up = jnp.concatenate([fields[group - 1][7:] if group else here[:1], here[:7]], axis=0)
            vertical = jnp.where(k + 1.0 < own, down - here, 0.0) + (up - here)
            tendency = horizontal_rate * sums[group] + vertical_rate * vertical
            base_v[pl.ds(group * 8, 8), at] = here + jnp.where(k < own, tracer_step * tendency, 0.0)
        return carry

    summed = zero
    for turn in range(ROUNDS):
        if turn == 1:
            arrive([tracer_link])
        if turn >= 1:
            lax.fori_loop(4 * (turn - 1), 4 * turn, tracer_block, 0)
        sums = gather(height, 0, own_columns(), [zero] * 6)
        arrive([functools.partial(height_link, turn)] + ([chosen_link] if turn == 0 else []))
        fields = [halo_height[turn, n] for n in range(4)]
        choices = [halo_chosen[n] for n in range(4)]
        picks = [pick(fields[n], choices[n]) for n in range(4)]
        halo = jnp.concatenate([picks[n][2 * n:2 * n + 2] for n in range(4)], axis=0)
        alive = jnp.concatenate([choices[n][2 * n:2 * n + 2] for n in range(4)], axis=0)
        sums = gather(halo, ROWS, own_columns(), sums)
        arrive([functools.partial(push_link, turn)] + ([near_link, weight_link] if turn == 0 else []))
        outer = jnp.concatenate([halo_push[turn, n] for n in range(4)], axis=0)

        def partner_columns(h):
            indices = [halo_near[h, slot] for slot in range(2)]
            return [(index >> 7, index & (BLOCK - 1)) for index in indices]

        found = []
        for h in range(4):
            got = gather(fields[h], 0, partner_columns(h), [zero] * 2)
            for g in range(4):
                gap = OFFSETS[h] + OFFSETS[g]
                if gap == 0 or gap in OFFSETS:
                    rows = picked if gap == 0 else picks[OFFSETS.index(gap)]
                    got = gather(rows[2 * g:2 * g + 2], ROWS + 2 * g, partner_columns(h), got)
            found.append(got)
        speed, height = own_update(sums, height, push)
        push = pushed_by(speed)
        summed = summed + speed
        sums = gather(height, 0, own_columns(), [zero] * 6)

        arrive([functools.partial(far_link, turn)], FAR)
        laplaces = []
        for h in range(4):
            for g in range(4):
                gap = OFFSETS[h] + OFFSETS[g]
                if gap in FAR:
                    f = FAR.index(gap)
                    at = PLACE[g] - FAR_ROWS[f][0]
                    rows = halo_three[turn, f, at] if f < 2 else halo_four[turn, f - 2, at]
                    found[h] = gather(rows, ROWS + 2 * g, partner_columns(h), found[h])
            for slot in range(2):
                place = 2 * h + slot
                difference = halo_weight[h, slot] * (found[h][slot] - spread(halo[place:place + 1]))
                laplaces.append(jnp.sum(difference, axis=0, keepdims=True))
        outer = outer + barotropic_step * jnp.concatenate(laplaces, axis=0)
        halo = jnp.where(alive >= 0, halo + barotropic_step * outer, 0.0)
        sums = gather(halo, ROWS, own_columns(), sums)
        speed, height = own_update(sums, height, push)
        push = pushed_by(speed)
        summed = summed + speed
        if turn < ROUNDS - 1:
            picked = put_round(turn + 1, height, push)
            begin([functools.partial(far_link, turn + 1)], FAR)
            begin([functools.partial(height_link, turn + 1), functools.partial(push_link, turn + 1)])
        if turn == 0:
            arrive([level_link])
            depths = gather(levels, 0, own_columns(), [zero] * 6)
            around = jnp.concatenate([halo_level[n] for n in range(4)], axis=0)
            depths = gather(around, ROWS, own_columns(), depths)
            for column in range(6):
                near_level[column] = depths[column]

    tail_v[0] = height
    tail_v[1] = speed
    tail_v[2] = summed * (1.0 / SUBSTEPS)
    for turn in range(ROUNDS):
        leave([functools.partial(far_link, turn)], FAR)
        leave([functools.partial(height_link, turn), functools.partial(push_link, turn)])
    leave([chosen_link, near_link, weight_link, level_link, tracer_link])


def finish(base_v, tail_v, tracer_out, ssh_out, velocity_out, result_v, out_sem):
    height_back = pltpu.make_async_copy(tail_v.at[0], ssh_out, out_sem.at[ROWS])
    speed_back = pltpu.make_async_copy(tail_v.at[1], velocity_out, out_sem.at[ROWS + 1])
    height_back.start()
    speed_back.start()
    mean = tail_v[2]
    levels = tail_v[3]
    level_f = lax.broadcasted_iota(jnp.int32, TILE, 0).astype(jnp.float32)
    shape = [tail_v[4 + group] for group in range(GROUPS)]
    backs = []
    for block in range(ROWS):
        own = spread(levels[block:block + 1])
        push = spread(mean[block:block + 1])
        for group in range(GROUPS):
            at = (pl.ds(group * 8, 8), cols(block))
            result_v[at] = base_v[at] + jnp.where(level_f + float(group * 8) < own, shape[group] * push, 0.0)
        if block % 4 == 3:
            half = pl.ds((block - 3) * BLOCK, 4 * BLOCK)
            backs.append(pltpu.make_async_copy(result_v.at[:, half], tracer_out.at[:, half], out_sem.at[block]))
            backs[-1].start()
    height_back.wait()
    speed_back.wait()
    for back in backs:
        back.wait()


def solution(mesh):
    parts = mesh.shape["dom"]

    def shards(tracer, bottom, near, weight, ssh, velocity, slots, thickness, profile):
        hbm = pl.BlockSpec(memory_space=pltpu.HBM)
        inner = pl.BlockSpec(memory_space=pltpu.VMEM)
        f32, i32 = jnp.float32, jnp.int32
        wide = (LEV, ROWS * BLOCK)
        dma = pltpu.SemaphoreType.DMA
        vmem, small = pltpu.VMEM, pltpu.SMEM
        levels = bottom.reshape(TILE)
        base, tail = pl.pallas_call(
            functools.partial(kernel, parts),
            out_shape=(vmem(wide, f32), vmem((4 + GROUPS, *TILE), f32)),
            in_specs=[hbm] * 9,
            out_specs=(inner, inner),
            scratch_shapes=[
                vmem(wide, f32), vmem(TILE, i32), vmem((6, ROWS * BLOCK), i32), vmem((6, ROWS * BLOCK), f32),
                vmem(TILE, f32), vmem(TILE, f32), small((1, 2, 4), i32), small((LEV,), f32), small((LEV,), f32),
                vmem((4, 2, LEV, BLOCK), f32), vmem((4, 2, LEV, BLOCK), f32),
                vmem((4, 2, BLOCK), f32), vmem((4, 2, BLOCK), f32), vmem(TILE, i32), vmem((4, *TILE), i32),
                vmem((4, 2, *TILE), i32), vmem((4, 2, *TILE), i32), vmem((4, 2, *TILE), f32), vmem((4, 2, *TILE), f32),
                vmem((ROUNDS, *TILE), f32), vmem((ROUNDS, 4, *TILE), f32),
                vmem((ROUNDS, 4, 2, BLOCK), f32), vmem((ROUNDS, 2, 2, 2, BLOCK), f32), vmem((ROUNDS, 2, 1, 2, BLOCK), f32),
                vmem((ROUNDS, 4, 2, BLOCK), f32), vmem((ROUNDS, 4, 2, BLOCK), f32),
                vmem((6, *TILE), i32), vmem((6, *TILE), i32), vmem((6, *TILE), f32), vmem((6, *TILE), f32), vmem(TILE, f32),
                dma((9,)), dma((4, 2)), dma((4, 2)), dma((4, 2)), dma((4, 2)), dma((4, 2)),
                dma((ROUNDS, 4, 2)), dma((ROUNDS, 4, 2)), dma((ROUNDS, 4, 2)),
            ],
            compiler_params=pltpu.CompilerParams(collective_id=0, has_side_effects=True),
        )(tracer, levels, near, weight, ssh.reshape(TILE), velocity.reshape(TILE), jnp.transpose(slots, (0, 2, 1)), thickness, profile)
        tile = jax.ShapeDtypeStruct(TILE, f32)
        out = pl.pallas_call(
            finish,
            out_shape=(jax.ShapeDtypeStruct(wide, f32), tile, tile),
            in_specs=[inner] * 2,
            out_specs=(hbm, hbm, hbm),
            scratch_shapes=[vmem(wide, f32), dma((ROWS + 2,))],
        )(*(pltpu.with_memory_space_constraint(x, pltpu.VMEM) for x in (base, tail)))
        return out[0], out[1].reshape(-1), out[2].reshape(-1)

    placed = (P(None, "dom"), P("dom"), P(None, "dom"), P(None, "dom"), P("dom"), P("dom"), P("dom", None, None), P(), P())
    return jax.shard_map(shards, mesh=mesh, in_specs=placed, out_specs=(P(None, "dom"), P("dom"), P("dom")), check_vma=False)
```

```python
import functools

import jax
import jax.numpy as jnp
from jax import lax
from jax.experimental import pallas as pl
from jax.experimental.pallas import tpu as pltpu
from jax.sharding import PartitionSpec as P

BLOCK = 128
ROWS = 8
LEV = 40
GROUPS = LEV // 8
SUBSTEPS = 6
OFFSETS = (1, -1, 2, -2)
horizontal_rate = 0.5
vertical_rate = 0.5
tracer_step = 0.2
barotropic_step = 0.5
friction = 0.05


FAR = (3, -3, 4, -4)
PLACE = (0, 2, 1, 3)
FAR_ROWS = ((0, 2), (2, 4), (1, 2), (3, 4))
ROUNDS = SUBSTEPS // 2
LAND = 2 * ROWS * BLOCK
TILE = (ROWS, BLOCK)


def along(values, index, axis):
    return jnp.take_along_axis(values, index, axis=axis, mode="promise_in_bounds")


def cols(block):
    return pl.ds(block * BLOCK, BLOCK)


def spread(row):
    return jnp.broadcast_to(row, TILE)


def kernel(
    parts, tracer_hbm, bottom_hbm, near_hbm, weight_hbm, ssh_hbm, velocity_hbm, slots_hbm, thickness_hbm, profile_hbm,
    base_v, tail_v,
    tracer_v, bottom_v, near_v, weight_v, ssh_v, velocity_v, slots, thickness, profile,
    send_tracer, halo_tracer, send_level, halo_level, send_chosen, halo_chosen,
    send_near, halo_near, send_weight, halo_weight, outer_row, outer_lane, outer_weight,
    send_height, halo_height, send_picked, halo_three, halo_four, send_push, halo_push,
    near_row, near_lane, weight_s, near_level, forcing_v,
    copy_sem, tracer_sem, level_sem, chosen_sem, near_sem, weight_sem, height_sem, far_sem, push_sem,
):
    me = lax.axis_index("dom")

    def start(source, target, number):
        copy = pltpu.make_async_copy(source, target, copy_sem.at[number])
        copy.start()
        return copy

    def inside(place):
        return (place >= 0) & (place < parts)

    barrier = pltpu.get_barrier_semaphore()
    for offset in OFFSETS + FAR:
        @pl.when(inside(me + offset))
        def _(offset=offset):
            pl.semaphore_signal(barrier, inc=1, device_id=(me + offset,), device_id_type=pl.DeviceIdType.MESH)

    slots_copy = start(slots_hbm, slots, 6)
    thickness_copy = start(thickness_hbm, thickness, 7)
    profile_copy = start(profile_hbm, profile, 8)
    tracer_copy = start(tracer_hbm, tracer_v, 4)
    bottom_copy = start(bottom_hbm, bottom_v, 1)
    near_copy = start(near_hbm, near_v, 2)
    weight_copy = start(weight_hbm, weight_v, 3)
    ssh_copy = start(ssh_hbm, ssh_v, 0)
    velocity_copy = start(velocity_hbm, velocity_v, 5)

    row_id = lax.broadcasted_iota(jnp.int32, TILE, 0)
    partner_id = row_id >> 1
    level_f = row_id.astype(jnp.float32)
    zero = jnp.zeros(TILE, jnp.float32)

    for number in range(4):
        @pl.when(jnp.logical_not(inside(me - OFFSETS[number])))
        def _(number=number):
            halo_chosen[number] = jnp.full(TILE, -1, jnp.int32)
            halo_near[number] = jnp.full((6, 2, BLOCK), LAND, jnp.int32)
            halo_weight[number] = jnp.zeros((6, 2, BLOCK), jnp.float32)
            halo_level[number] = jnp.zeros((2, BLOCK), jnp.float32)
            halo_tracer[number] = jnp.zeros((2, LEV, BLOCK), jnp.float32)
            for turn in range(ROUNDS):
                halo_height[turn, number] = zero
                halo_push[turn, number] = jnp.zeros((2, BLOCK), jnp.float32)
        @pl.when(jnp.logical_not(inside(me - FAR[number])))
        def _(number=number):
            for turn in range(ROUNDS):
                if number < 2:
                    halo_three[turn, number] = jnp.zeros((2, 2, BLOCK), jnp.float32)
                else:
                    halo_four[turn, number - 2] = jnp.zeros((1, 2, BLOCK), jnp.float32)

    def remote(source, target, sems, offset):
        return pltpu.make_async_remote_copy(
            src_ref=source, dst_ref=target, send_sem=sems.at[0], recv_sem=sems.at[1],
            device_id=(me + offset,), device_id_type=pl.DeviceIdType.MESH)

    def tracer_link(n):
        return remote(send_tracer.at[n], halo_tracer.at[n], tracer_sem.at[n], OFFSETS[n])

    def level_link(n):
        return remote(send_level.at[n], halo_level.at[n], level_sem.at[n], OFFSETS[n])

    def chosen_link(n):
        return remote(send_chosen, halo_chosen.at[n], chosen_sem.at[n], OFFSETS[n])

    def near_link(n):
        return remote(send_near.at[n], halo_near.at[n], near_sem.at[n], OFFSETS[n])

    def weight_link(n):
        return remote(send_weight.at[n], halo_weight.at[n], weight_sem.at[n], OFFSETS[n])

    def height_link(turn, n):
        return remote(send_height.at[turn], halo_height.at[turn, n], height_sem.at[turn, n], OFFSETS[n])

    def push_link(turn, n):
        return remote(send_push.at[turn, n], halo_push.at[turn, n], push_sem.at[turn, n], OFFSETS[n])

    def far_link(turn, n):
        low, high = FAR_ROWS[n]
        target = halo_three.at[turn, n] if n < 2 else halo_four.at[turn, n - 2]
        return remote(send_picked.at[turn, pl.ds(low, high - low)], target, far_sem.at[turn, n], FAR[n])

    def begin(links, offsets=OFFSETS):
        for number in range(4):
            @pl.when(inside(me + offsets[number]))
            def _(number=number):
                for link in links:
                    link(number).start()

    def arrive(links, offsets=OFFSETS):
        for number in range(4):
            @pl.when(inside(me - offsets[number]))
            def _(number=number):
                for link in links:
                    link(number).wait_recv()

    def leave(links, offsets=OFFSETS):
        for number in range(4):
            @pl.when(inside(me + offsets[number]))
            def _(number=number):
                for link in links:
                    link(number).wait_send()

    slots_copy.wait()
    chosen = zero.astype(jnp.int32)
    for number in range(4):
        for slot in range(2):
            chosen = jnp.where(row_id == 2 * number + slot, slots[0, slot, number], chosen)
    send_chosen[...] = chosen

    def pick(values, choice):
        return jnp.where(choice >= 0, along(values, jnp.maximum(choice, 0), 0), 0.0)

    def put_round(turn, height, push):
        picked = pick(height, chosen)
        pushed = pick(push, chosen)
        send_height[turn] = height
        for number in range(4):
            send_picked[turn, PLACE[number]] = picked[2 * number:2 * number + 2]
            send_push[turn, number] = pushed[2 * number:2 * number + 2]
        return picked

    bottom_copy.wait()
    levels = bottom_v[...].astype(jnp.float32)
    sent_levels = pick(levels, chosen)
    for number in range(4):
        send_level[number] = sent_levels[2 * number:2 * number + 2]
    thickness_copy.wait()
    profile_copy.wait()
    thick = []
    for group in range(GROUPS):
        t, p = zero, zero
        for k in range(8):
            t = jnp.where(row_id == k, thickness[group * 8 + k], t)
            p = jnp.where(row_id == k, profile[group * 8 + k], p)
        thick.append(t)
        tail_v[4 + group] = p
    tail_v[3] = levels
    tracer_copy.wait()
    for block in range(ROWS):
        own = spread(levels[block:block + 1])
        top, under = zero, zero
        for group in range(GROUPS):
            layer = jnp.where(level_f + float(group * 8) < own, thick[group], 0.0)
            top = top + layer * tracer_v[pl.ds(group * 8, 8), cols(block)]
            under = under + layer
        forcing_v[block:block + 1] = jnp.sum(top, axis=0, keepdims=True) / jnp.sum(under, axis=0, keepdims=True)
    forcing = forcing_v[...]
    ssh_copy.wait()
    velocity_copy.wait()
    height = ssh_v[...]

    def pushed_by(speed):
        return (1.0 - friction) * speed + barotropic_step * forcing

    push = pushed_by(velocity_v[...])
    picked = put_round(0, height, push)

    near_copy.wait()
    weight_copy.wait()
    total_weight = zero
    for column in range(6):
        for block in range(ROWS):
            near_row[column, block:block + 1] = near_v[column:column + 1, cols(block)]
            weight_s[column, block:block + 1] = weight_v[column:column + 1, cols(block)]
    for column in range(6):
        index = near_row[column]
        weight = weight_s[column]
        total_weight = total_weight + weight
        sent_index = along(index, jnp.maximum(chosen, 0), 0)
        sent_weight = pick(weight, chosen)
        for number in range(4):
            send_near[number, column] = sent_index[2 * number:2 * number + 2]
            send_weight[number, column] = sent_weight[2 * number:2 * number + 2]
        near_lane[column] = index & (BLOCK - 1)
        near_row[column] = index >> 7
    for place in range(ROWS):
        which = spread(chosen[place:place + 1])
        for group in range(GROUPS):
            piece = zero
            for block in range(ROWS):
                piece = jnp.where(which == block, tracer_v[pl.ds(group * 8, 8), cols(block)], piece)
            send_tracer[place // 2, place % 2, pl.ds(group * 8, 8), :] = piece

    pl.semaphore_wait(barrier, sum(inside(me + offset).astype(jnp.int32) for offset in OFFSETS + FAR))
    begin([functools.partial(height_link, 0)])
    begin([chosen_link])
    begin([functools.partial(far_link, 0)], FAR)
    begin([near_link, weight_link])
    begin([functools.partial(push_link, 0)])
    begin([level_link, tracer_link])

    def gather(rows, first_row, columns, sums):
        sums = list(sums)
        count = rows.shape[0]
        wide = [spread(rows[r:r + 1]) for r in range(count)]
        for i, (row, lane) in enumerate(columns):
            for r in range(count):
                sums[i] = jnp.where(row == first_row + r, along(wide[r], lane, 1), sums[i])
        return sums

    def own_columns():
        return [(near_row[column], near_lane[column]) for column in range(6)]

    def own_update(sums, height, push):
        laplace = -total_weight * height
        for column in range(6):
            laplace = laplace + weight_s[column] * sums[column]
        speed = push + barotropic_step * laplace
        return speed, height + barotropic_step * speed

    def tracer_block(block, carry):
        at = pl.ds(pl.multiple_of(block * BLOCK, BLOCK), BLOCK)
        fields = [tracer_v[pl.ds(group * 8, 8), at] for group in range(GROUPS)]
        own = spread(bottom_v[pl.ds(block, 1), :].astype(jnp.float32))
        sums = [zero] * GROUPS
        for column in range(6):
            index = spread(near_v[column:column + 1, at])
            weight = spread(weight_v[column:column + 1, at])
            depth = spread(near_level[column, pl.ds(block, 1), :])
            lane = index & (BLOCK - 1)
            row = index >> 7
            got = [zero] * GROUPS
            for r in range(2 * ROWS):
                here = row == r
                for group in range(GROUPS):
                    if r < ROWS:
                        table = tracer_v[pl.ds(group * 8, 8), cols(r)]
                    else:
                        table = halo_tracer[(r - ROWS) // 2, (r - ROWS) % 2, pl.ds(group * 8, 8), :]
                    got[group] = jnp.where(here, along(table, lane, 1), got[group])
            for group in range(GROUPS):
                wet = jnp.where(level_f + float(group * 8) < depth, weight, 0.0)
                sums[group] = sums[group] + wet * (got[group] - fields[group])
        for group in range(GROUPS):
            here = fields[group]
            k = level_f + float(group * 8)
            down = jnp.concatenate([here[1:], fields[group + 1][:1] if group < GROUPS - 1 else here[7:]], axis=0)
            up = jnp.concatenate([fields[group - 1][7:] if group else here[:1], here[:7]], axis=0)
            vertical = jnp.where(k + 1.0 < own, down - here, 0.0) + (up - here)
            tendency = horizontal_rate * sums[group] + vertical_rate * vertical
            base_v[pl.ds(group * 8, 8), at] = here + jnp.where(k < own, tracer_step * tendency, 0.0)
        return carry

    summed = zero
    for turn in range(ROUNDS):
        if turn == 1:
            arrive([tracer_link])
        if turn >= 1:
            lax.fori_loop(4 * (turn - 1), 4 * turn, tracer_block, 0)
        sums = gather(height, 0, own_columns(), [zero] * 6)
        if turn == ROUNDS - 1:
            leave([chosen_link, near_link, weight_link, level_link, tracer_link])
            for earlier in range(ROUNDS):
                leave([functools.partial(far_link, earlier)], FAR)
                leave([functools.partial(height_link, earlier), functools.partial(push_link, earlier)])
        arrive([functools.partial(height_link, turn), functools.partial(push_link, turn)] + ([chosen_link, near_link, weight_link] if turn == 0 else []))
        if turn == 0:
            for column in range(6):
                index = jnp.concatenate([halo_near[n, column] for n in range(4)], axis=0)
                outer_lane[column] = index & (BLOCK - 1)
                outer_row[column] = index >> 7
                outer_weight[column] = jnp.concatenate([halo_weight[n, column] for n in range(4)], axis=0)
        fields = [halo_height[turn, n] for n in range(4)]
        choices = [halo_chosen[n] for n in range(4)]
        picks = [pick(fields[n], choices[n]) for n in range(4)]
        halo = jnp.concatenate([picks[n][2 * n:2 * n + 2] for n in range(4)], axis=0)
        alive = jnp.concatenate([choices[n][2 * n:2 * n + 2] for n in range(4)], axis=0)
        sums = gather(halo, ROWS, own_columns(), sums)

        def mixed(rows):
            tile = zero
            for h in range(4):
                if rows[h] is not None:
                    tile = jnp.where(partner_id == h, spread(rows[h]), tile)
            return tile

        def outer_gather(tiles):
            found = [zero] * 6
            for column in range(6):
                row = outer_row[column]
                lane = outer_lane[column]
                for r, tile in tiles:
                    found[column] = jnp.where(row == r, along(tile, lane, 1), found[column])
            total = zero
            for column in range(6):
                total = total + outer_weight[column] * found[column]
            return total

        tiles = [(r, mixed([fields[h][r:r + 1] for h in range(4)])) for r in range(ROWS)]
        for g in range(4):
            gaps = [OFFSETS[h] + OFFSETS[g] for h in range(4)]
            for slot in range(2):
                at = 2 * g + slot
                rows = [picked[at:at + 1] if gap == 0 else picks[OFFSETS.index(gap)][at:at + 1] if gap in OFFSETS else None for gap in gaps]
                tiles.append((ROWS + at, mixed(rows)))
        outer = jnp.concatenate([halo_push[turn, n] for n in range(4)], axis=0)
        weight = zero
        for column in range(6):
            weight = weight + outer_weight[column]
        outer = outer + barotropic_step * (outer_gather(tiles) - weight * halo)
        speed, height = own_update(sums, height, push)
        push = pushed_by(speed)
        summed = summed + speed
        sums = gather(height, 0, own_columns(), [zero] * 6)

        arrive([functools.partial(far_link, turn)], FAR)
        tiles = []
        for g in range(4):
            gaps = [OFFSETS[h] + OFFSETS[g] for h in range(4)]
            for slot in range(2):
                rows = []
                for gap in gaps:
                    if gap in FAR:
                        f = FAR.index(gap)
                        at = PLACE[g] - FAR_ROWS[f][0]
                        rows.append((halo_three[turn, f, at] if f < 2 else halo_four[turn, f - 2, at])[slot:slot + 1])
                    else:
                        rows.append(None)
                tiles.append((ROWS + 2 * g + slot, mixed(rows)))
        outer = outer + barotropic_step * outer_gather(tiles)
        halo = jnp.where(alive >= 0, halo + barotropic_step * outer, 0.0)
        sums = gather(halo, ROWS, own_columns(), sums)
        speed, height = own_update(sums, height, push)
        push = pushed_by(speed)
        summed = summed + speed
        if turn < ROUNDS - 1:
            picked = put_round(turn + 1, height, push)
            begin([functools.partial(height_link, turn + 1)])
            begin([functools.partial(far_link, turn + 1)], FAR)
            begin([functools.partial(push_link, turn + 1)])
        if turn == 0:
            arrive([level_link])
            depths = gather(levels, 0, own_columns(), [zero] * 6)
            around = jnp.concatenate([halo_level[n] for n in range(4)], axis=0)
            depths = gather(around, ROWS, own_columns(), depths)
            for column in range(6):
                near_level[column] = depths[column]

    tail_v[0] = height
    tail_v[1] = speed
    tail_v[2] = summed * (1.0 / SUBSTEPS)


def finish(base_v, tail_v, tracer_out, ssh_out, velocity_out, result_v, out_sem):
    height_back = pltpu.make_async_copy(tail_v.at[0], ssh_out, out_sem.at[ROWS])
    speed_back = pltpu.make_async_copy(tail_v.at[1], velocity_out, out_sem.at[ROWS + 1])
    height_back.start()
    speed_back.start()
    mean = tail_v[2]
    levels = tail_v[3]
    level_f = lax.broadcasted_iota(jnp.int32, TILE, 0).astype(jnp.float32)
    shape = [tail_v[4 + group] for group in range(GROUPS)]
    backs = []
    for block in range(ROWS):
        own = spread(levels[block:block + 1])
        push = spread(mean[block:block + 1])
        for group in range(GROUPS):
            at = (pl.ds(group * 8, 8), cols(block))
            result_v[at] = base_v[at] + jnp.where(level_f + float(group * 8) < own, shape[group] * push, 0.0)
        if block % 4 == 3:
            half = pl.ds((block - 3) * BLOCK, 4 * BLOCK)
            backs.append(pltpu.make_async_copy(result_v.at[:, half], tracer_out.at[:, half], out_sem.at[block]))
            backs[-1].start()
    height_back.wait()
    speed_back.wait()
    for back in backs:
        back.wait()


def solution(mesh):
    parts = mesh.shape["dom"]

    def shards(tracer, bottom, near, weight, ssh, velocity, slots, thickness, profile):
        hbm = pl.BlockSpec(memory_space=pltpu.HBM)
        inner = pl.BlockSpec(memory_space=pltpu.VMEM)
        f32, i32 = jnp.float32, jnp.int32
        wide = (LEV, ROWS * BLOCK)
        dma = pltpu.SemaphoreType.DMA
        vmem, small = pltpu.VMEM, pltpu.SMEM
        levels = bottom.reshape(TILE)
        base, tail = pl.pallas_call(
            functools.partial(kernel, parts),
            out_shape=(vmem(wide, f32), vmem((4 + GROUPS, *TILE), f32)),
            in_specs=[hbm] * 9,
            out_specs=(inner, inner),
            scratch_shapes=[
                vmem(wide, f32), vmem(TILE, i32), vmem((6, ROWS * BLOCK), i32), vmem((6, ROWS * BLOCK), f32),
                vmem(TILE, f32), vmem(TILE, f32), small((1, 2, 4), i32), small((LEV,), f32), small((LEV,), f32),
                vmem((4, 2, LEV, BLOCK), f32), vmem((4, 2, LEV, BLOCK), f32),
                vmem((4, 2, BLOCK), f32), vmem((4, 2, BLOCK), f32), vmem(TILE, i32), vmem((4, *TILE), i32),
                vmem((4, 6, 2, BLOCK), i32), vmem((4, 6, 2, BLOCK), i32), vmem((4, 6, 2, BLOCK), f32), vmem((4, 6, 2, BLOCK), f32),
                vmem((6, *TILE), i32), vmem((6, *TILE), i32), vmem((6, *TILE), f32),
                vmem((ROUNDS, *TILE), f32), vmem((ROUNDS, 4, *TILE), f32),
                vmem((ROUNDS, 4, 2, BLOCK), f32), vmem((ROUNDS, 2, 2, 2, BLOCK), f32), vmem((ROUNDS, 2, 1, 2, BLOCK), f32),
                vmem((ROUNDS, 4, 2, BLOCK), f32), vmem((ROUNDS, 4, 2, BLOCK), f32),
                vmem((6, *TILE), i32), vmem((6, *TILE), i32), vmem((6, *TILE), f32), vmem((6, *TILE), f32), vmem(TILE, f32),
                dma((9,)), dma((4, 2)), dma((4, 2)), dma((4, 2)), dma((4, 2)), dma((4, 2)),
                dma((ROUNDS, 4, 2)), dma((ROUNDS, 4, 2)), dma((ROUNDS, 4, 2)),
            ],
            compiler_params=pltpu.CompilerParams(collective_id=0, has_side_effects=True),
        )(tracer, levels, near, weight, ssh.reshape(TILE), velocity.reshape(TILE), jnp.transpose(slots, (0, 2, 1)), thickness, profile)
        tile = jax.ShapeDtypeStruct(TILE, f32)
        out = pl.pallas_call(
            finish,
            out_shape=(jax.ShapeDtypeStruct(wide, f32), tile, tile),
            in_specs=[inner] * 2,
            out_specs=(hbm, hbm, hbm),
            scratch_shapes=[vmem(wide, f32), dma((ROWS + 2,))],
        )(*(pltpu.with_memory_space_constraint(x, pltpu.VMEM) for x in (base, tail)))
        return out[0], out[1].reshape(-1), out[2].reshape(-1)

    placed = (P(None, "dom"), P("dom"), P(None, "dom"), P(None, "dom"), P("dom"), P("dom"), P("dom", None, None), P(), P())
    return jax.shard_map(shards, mesh=mesh, in_specs=placed, out_specs=(P(None, "dom"), P("dom"), P("dom")), check_vma=False)
```

```python
import functools

import jax
import jax.numpy as jnp
from jax import lax
from jax.experimental import pallas as pl
from jax.experimental.pallas import tpu as pltpu
from jax.sharding import PartitionSpec as P

BLOCK = 128
ROWS = 8
LEV = 40
GROUPS = LEV // 8
SUBSTEPS = 6
OFFSETS = (1, -1, 2, -2)
horizontal_rate = 0.5
vertical_rate = 0.5
tracer_step = 0.2
barotropic_step = 0.5
friction = 0.05


FAR = (3, -3, 4, -4)
PLACE = (0, 2, 1, 3)
FAR_ROWS = ((0, 2), (2, 4), (1, 2), (3, 4))
ROUNDS = SUBSTEPS // 2
LAND = 2 * ROWS * BLOCK
TILE = (ROWS, BLOCK)


def along(values, index, axis):
    return jnp.take_along_axis(values, index, axis=axis, mode="promise_in_bounds")


def cols(block):
    return pl.ds(block * BLOCK, BLOCK)


def spread(row):
    return jnp.broadcast_to(row, TILE)


def kernel(
    parts, tracer_hbm, bottom_hbm, near_hbm, weight_hbm, ssh_hbm, velocity_hbm, slots_hbm, thickness_hbm, profile_hbm,
    base_v, tail_v,
    tracer_v, bottom_v, near_v, weight_v, ssh_v, velocity_v, slots, thickness, profile,
    send_tracer, halo_tracer,
    send_whole, halo_whole, send_real, halo_real, outer_row, outer_lane, outer_weight,
    send_height, halo_height, send_picked, halo_three, halo_four,
    near_row, near_lane, weight_s, near_level, forcing_v,
    copy_sem, tracer_sem, whole_sem, real_sem, height_sem, far_sem,
):
    me = lax.axis_index("dom")

    def start(source, target, number):
        copy = pltpu.make_async_copy(source, target, copy_sem.at[number])
        copy.start()
        return copy

    def inside(place):
        return (place >= 0) & (place < parts)

    barrier = pltpu.get_barrier_semaphore()
    for offset in OFFSETS + FAR:
        @pl.when(inside(me + offset))
        def _(offset=offset):
            pl.semaphore_signal(barrier, inc=1, device_id=(me + offset,), device_id_type=pl.DeviceIdType.MESH)

    slots_copy = start(slots_hbm, slots, 6)
    thickness_copy = start(thickness_hbm, thickness, 7)
    profile_copy = start(profile_hbm, profile, 8)
    tracer_copy = start(tracer_hbm, tracer_v, 4)
    bottom_copy = start(bottom_hbm, bottom_v, 1)
    near_copy = start(near_hbm, near_v, 2)
    weight_copy = start(weight_hbm, weight_v, 3)
    ssh_copy = start(ssh_hbm, ssh_v, 0)
    velocity_copy = start(velocity_hbm, velocity_v, 5)

    row_id = lax.broadcasted_iota(jnp.int32, TILE, 0)
    partner_id = row_id >> 1
    level_f = row_id.astype(jnp.float32)
    zero = jnp.zeros(TILE, jnp.float32)

    for number in range(4):
        @pl.when(jnp.logical_not(inside(me - OFFSETS[number])))
        def _(number=number):
            halo_whole[number, 0:ROWS] = jnp.full(TILE, -1, jnp.int32)
            halo_whole[number, ROWS:ROWS + 12] = jnp.full((12, BLOCK), LAND, jnp.int32)
            halo_real[number] = jnp.zeros((14, BLOCK), jnp.float32)
            halo_tracer[number] = jnp.zeros((2, LEV, BLOCK), jnp.float32)
            for turn in range(ROUNDS):
                halo_height[turn, number] = jnp.zeros((ROWS + 2, BLOCK), jnp.float32)
        @pl.when(jnp.logical_not(inside(me - FAR[number])))
        def _(number=number):
            for turn in range(ROUNDS):
                if number < 2:
                    halo_three[turn, number] = jnp.zeros((2, 2, BLOCK), jnp.float32)
                else:
                    halo_four[turn, number - 2] = jnp.zeros((1, 2, BLOCK), jnp.float32)

    def remote(source, target, sems, offset):
        return pltpu.make_async_remote_copy(
            src_ref=source, dst_ref=target, send_sem=sems.at[0], recv_sem=sems.at[1],
            device_id=(me + offset,), device_id_type=pl.DeviceIdType.MESH)

    def tracer_link(n):
        return remote(send_tracer.at[n], halo_tracer.at[n], tracer_sem.at[n], OFFSETS[n])

    def whole_link(n):
        return remote(send_whole.at[n], halo_whole.at[n], whole_sem.at[n], OFFSETS[n])

    def real_link(n):
        return remote(send_real.at[n], halo_real.at[n], real_sem.at[n], OFFSETS[n])

    def height_link(turn, n):
        return remote(send_height.at[turn, n], halo_height.at[turn, n], height_sem.at[turn, n], OFFSETS[n])

    def far_link(turn, n):
        low, high = FAR_ROWS[n]
        target = halo_three.at[turn, n] if n < 2 else halo_four.at[turn, n - 2]
        return remote(send_picked.at[turn, pl.ds(low, high - low)], target, far_sem.at[turn, n], FAR[n])

    def begin(links, offsets=OFFSETS):
        for number in range(4):
            @pl.when(inside(me + offsets[number]))
            def _(number=number):
                for link in links:
                    link(number).start()

    def arrive(links, offsets=OFFSETS):
        for number in range(4):
            @pl.when(inside(me - offsets[number]))
            def _(number=number):
                for link in links:
                    link(number).wait_recv()

    def leave(links, offsets=OFFSETS):
        for number in range(4):
            @pl.when(inside(me + offsets[number]))
            def _(number=number):
                for link in links:
                    link(number).wait_send()

    slots_copy.wait()
    chosen = zero.astype(jnp.int32)
    for number in range(4):
        for slot in range(2):
            chosen = jnp.where(row_id == 2 * number + slot, slots[0, slot, number], chosen)
    for number in range(4):
        send_whole[number, 0:ROWS] = chosen

    def pick(values, choice):
        return jnp.where(choice >= 0, along(values, jnp.maximum(choice, 0), 0), 0.0)

    def put_round(turn, height, push):
        picked = pick(height, chosen)
        pushed = pick(push, chosen)
        for number in range(4):
            send_picked[turn, PLACE[number]] = picked[2 * number:2 * number + 2]
            send_height[turn, number, 0:ROWS] = height
            send_height[turn, number, ROWS:ROWS + 2] = pushed[2 * number:2 * number + 2]
        return picked

    bottom_copy.wait()
    levels = bottom_v[...].astype(jnp.float32)
    sent_levels = pick(levels, chosen)
    for number in range(4):
        send_real[number, 12:14] = sent_levels[2 * number:2 * number + 2]
    thickness_copy.wait()
    profile_copy.wait()
    thick = []
    for group in range(GROUPS):
        t, p = zero, zero
        for k in range(8):
            t = jnp.where(row_id == k, thickness[group * 8 + k], t)
            p = jnp.where(row_id == k, profile[group * 8 + k], p)
        thick.append(t)
        tail_v[4 + group] = p
    tail_v[3] = levels
    tracer_copy.wait()
    for block in range(ROWS):
        own = spread(levels[block:block + 1])
        top, under = zero, zero
        for group in range(GROUPS):
            layer = jnp.where(level_f + float(group * 8) < own, thick[group], 0.0)
            top = top + layer * tracer_v[pl.ds(group * 8, 8), cols(block)]
            under = under + layer
        forcing_v[block:block + 1] = jnp.sum(top, axis=0, keepdims=True) / jnp.sum(under, axis=0, keepdims=True)
    forcing = forcing_v[...]
    ssh_copy.wait()
    velocity_copy.wait()
    height = ssh_v[...]

    def pushed_by(speed):
        return (1.0 - friction) * speed + barotropic_step * forcing

    push = pushed_by(velocity_v[...])
    picked = put_round(0, height, push)

    near_copy.wait()
    weight_copy.wait()
    total_weight = zero
    for column in range(6):
        for block in range(ROWS):
            near_row[column, block:block + 1] = near_v[column:column + 1, cols(block)]
            weight_s[column, block:block + 1] = weight_v[column:column + 1, cols(block)]
    for column in range(6):
        index = near_row[column]
        weight = weight_s[column]
        total_weight = total_weight + weight
        sent_index = along(index, jnp.maximum(chosen, 0), 0)
        sent_weight = pick(weight, chosen)
        for number in range(4):
            send_whole[number, ROWS + 2 * column:ROWS + 2 * column + 2] = sent_index[2 * number:2 * number + 2]
            send_real[number, 2 * column:2 * column + 2] = sent_weight[2 * number:2 * number + 2]
        near_lane[column] = index & (BLOCK - 1)
        near_row[column] = index >> 7
    for place in range(ROWS):
        which = spread(chosen[place:place + 1])
        for group in range(GROUPS):
            piece = zero
            for block in range(ROWS):
                piece = jnp.where(which == block, tracer_v[pl.ds(group * 8, 8), cols(block)], piece)
            send_tracer[place // 2, place % 2, pl.ds(group * 8, 8), :] = piece

    pl.semaphore_wait(barrier, sum(inside(me + offset).astype(jnp.int32) for offset in OFFSETS + FAR))
    begin([functools.partial(height_link, 0)])
    begin([functools.partial(far_link, 0)], FAR)
    begin([whole_link, real_link])
    begin([tracer_link])

    def gather(rows, first_row, columns, sums):
        sums = list(sums)
        count = rows.shape[0]
        wide = [spread(rows[r:r + 1]) for r in range(count)]
        for i, (row, lane) in enumerate(columns):
            for r in range(count):
                sums[i] = jnp.where(row == first_row + r, along(wide[r], lane, 1), sums[i])
        return sums

    def own_columns():
        return [(near_row[column], near_lane[column]) for column in range(6)]

    def own_update(sums, height, push):
        laplace = -total_weight * height
        for column in range(6):
            laplace = laplace + weight_s[column] * sums[column]
        speed = push + barotropic_step * laplace
        return speed, height + barotropic_step * speed

    def tracer_block(block, carry):
        at = pl.ds(pl.multiple_of(block * BLOCK, BLOCK), BLOCK)
        fields = [tracer_v[pl.ds(group * 8, 8), at] for group in range(GROUPS)]
        own = spread(bottom_v[pl.ds(block, 1), :].astype(jnp.float32))
        sums = [zero] * GROUPS
        for column in range(6):
            index = spread(near_v[column:column + 1, at])
            weight = spread(weight_v[column:column + 1, at])
            depth = spread(near_level[column, pl.ds(block, 1), :])
            lane = index & (BLOCK - 1)
            row = index >> 7
            got = [zero] * GROUPS
            for r in range(2 * ROWS):
                here = row == r
                for group in range(GROUPS):
                    if r < ROWS:
                        table = tracer_v[pl.ds(group * 8, 8), cols(r)]
                    else:
                        table = halo_tracer[(r - ROWS) // 2, (r - ROWS) % 2, pl.ds(group * 8, 8), :]
                    got[group] = jnp.where(here, along(table, lane, 1), got[group])
            for group in range(GROUPS):
                wet = jnp.where(level_f + float(group * 8) < depth, weight, 0.0)
                sums[group] = sums[group] + wet * (got[group] - fields[group])
        for group in range(GROUPS):
            here = fields[group]
            k = level_f + float(group * 8)
            down = jnp.concatenate([here[1:], fields[group + 1][:1] if group < GROUPS - 1 else here[7:]], axis=0)
            up = jnp.concatenate([fields[group - 1][7:] if group else here[:1], here[:7]], axis=0)
            vertical = jnp.where(k + 1.0 < own, down - here, 0.0) + (up - here)
            tendency = horizontal_rate * sums[group] + vertical_rate * vertical
            base_v[pl.ds(group * 8, 8), at] = here + jnp.where(k < own, tracer_step * tendency, 0.0)
        return carry

    summed = zero
    for turn in range(ROUNDS):
        if turn == 1:
            arrive([tracer_link])
        if turn >= 1:
            lax.fori_loop(4 * (turn - 1), 4 * turn, tracer_block, 0)
        sums = gather(height, 0, own_columns(), [zero] * 6)
        if turn == ROUNDS - 1:
            leave([whole_link, real_link, tracer_link])
            for earlier in range(ROUNDS):
                leave([functools.partial(far_link, earlier)], FAR)
                leave([functools.partial(height_link, earlier)])
        arrive([functools.partial(height_link, turn)] + ([whole_link, real_link] if turn == 0 else []))
        if turn == 0:
            for column in range(6):
                index = jnp.concatenate([halo_whole[n, ROWS + 2 * column:ROWS + 2 * column + 2] for n in range(4)], axis=0)
                outer_lane[column] = index & (BLOCK - 1)
                outer_row[column] = index >> 7
                outer_weight[column] = jnp.concatenate([halo_real[n, 2 * column:2 * column + 2] for n in range(4)], axis=0)
        fields = [halo_height[turn, n, 0:ROWS] for n in range(4)]
        choices = [halo_whole[n, 0:ROWS] for n in range(4)]
        picks = [pick(fields[n], choices[n]) for n in range(4)]
        halo = jnp.concatenate([picks[n][2 * n:2 * n + 2] for n in range(4)], axis=0)
        alive = jnp.concatenate([choices[n][2 * n:2 * n + 2] for n in range(4)], axis=0)
        sums = gather(halo, ROWS, own_columns(), sums)

        def mixed(rows):
            tile = zero
            for h in range(4):
                if rows[h] is not None:
                    tile = jnp.where(partner_id == h, spread(rows[h]), tile)
            return tile

        def outer_gather(tiles):
            found = [zero] * 6
            for column in range(6):
                row = outer_row[column]
                lane = outer_lane[column]
                for r, tile in tiles:
                    found[column] = jnp.where(row == r, along(tile, lane, 1), found[column])
            total = zero
            for column in range(6):
                total = total + outer_weight[column] * found[column]
            return total

        tiles = [(r, mixed([fields[h][r:r + 1] for h in range(4)])) for r in range(ROWS)]
        for g in range(4):
            gaps = [OFFSETS[h] + OFFSETS[g] for h in range(4)]
            for slot in range(2):
                at = 2 * g + slot
                rows = [picked[at:at + 1] if gap == 0 else picks[OFFSETS.index(gap)][at:at + 1] if gap in OFFSETS else None for gap in gaps]
                tiles.append((ROWS + at, mixed(rows)))
        outer = jnp.concatenate([halo_height[turn, n, ROWS:ROWS + 2] for n in range(4)], axis=0)
        weight = zero
        for column in range(6):
            weight = weight + outer_weight[column]
        outer = outer + barotropic_step * (outer_gather(tiles) - weight * halo)
        speed, height = own_update(sums, height, push)
        push = pushed_by(speed)
        summed = summed + speed
        sums = gather(height, 0, own_columns(), [zero] * 6)

        arrive([functools.partial(far_link, turn)], FAR)
        tiles = []
        for g in range(4):
            gaps = [OFFSETS[h] + OFFSETS[g] for h in range(4)]
            for slot in range(2):
                rows = []
                for gap in gaps:
                    if gap in FAR:
                        f = FAR.index(gap)
                        at = PLACE[g] - FAR_ROWS[f][0]
                        rows.append((halo_three[turn, f, at] if f < 2 else halo_four[turn, f - 2, at])[slot:slot + 1])
                    else:
                        rows.append(None)
                tiles.append((ROWS + 2 * g + slot, mixed(rows)))
        outer = outer + barotropic_step * outer_gather(tiles)
        halo = jnp.where(alive >= 0, halo + barotropic_step * outer, 0.0)
        sums = gather(halo, ROWS, own_columns(), sums)
        speed, height = own_update(sums, height, push)
        push = pushed_by(speed)
        summed = summed + speed
        if turn < ROUNDS - 1:
            picked = put_round(turn + 1, height, push)
            begin([functools.partial(height_link, turn + 1)])
            begin([functools.partial(far_link, turn + 1)], FAR)
        if turn == 0:
            depths = gather(levels, 0, own_columns(), [zero] * 6)
            around = jnp.concatenate([halo_real[n, 12:14] for n in range(4)], axis=0)
            depths = gather(around, ROWS, own_columns(), depths)
            for column in range(6):
                near_level[column] = depths[column]

    tail_v[0] = height
    tail_v[1] = speed
    tail_v[2] = summed * (1.0 / SUBSTEPS)


def finish(base_v, tail_v, tracer_out, ssh_out, velocity_out, result_v, out_sem):
    height_back = pltpu.make_async_copy(tail_v.at[0], ssh_out, out_sem.at[ROWS])
    speed_back = pltpu.make_async_copy(tail_v.at[1], velocity_out, out_sem.at[ROWS + 1])
    height_back.start()
    speed_back.start()
    mean = tail_v[2]
    levels = tail_v[3]
    level_f = lax.broadcasted_iota(jnp.int32, TILE, 0).astype(jnp.float32)
    shape = [tail_v[4 + group] for group in range(GROUPS)]
    backs = []
    for block in range(ROWS):
        own = spread(levels[block:block + 1])
        push = spread(mean[block:block + 1])
        for group in range(GROUPS):
            at = (pl.ds(group * 8, 8), cols(block))
            result_v[at] = base_v[at] + jnp.where(level_f + float(group * 8) < own, shape[group] * push, 0.0)
        if block % 4 == 3:
            half = pl.ds((block - 3) * BLOCK, 4 * BLOCK)
            backs.append(pltpu.make_async_copy(result_v.at[:, half], tracer_out.at[:, half], out_sem.at[block]))
            backs[-1].start()
    height_back.wait()
    speed_back.wait()
    for back in backs:
        back.wait()


def solution(mesh):
    parts = mesh.shape["dom"]

    def shards(tracer, bottom, near, weight, ssh, velocity, slots, thickness, profile):
        hbm = pl.BlockSpec(memory_space=pltpu.HBM)
        inner = pl.BlockSpec(memory_space=pltpu.VMEM)
        f32, i32 = jnp.float32, jnp.int32
        wide = (LEV, ROWS * BLOCK)
        dma = pltpu.SemaphoreType.DMA
        vmem, small = pltpu.VMEM, pltpu.SMEM
        levels = bottom.reshape(TILE)
        base, tail = pl.pallas_call(
            functools.partial(kernel, parts),
            out_shape=(vmem(wide, f32), vmem((4 + GROUPS, *TILE), f32)),
            in_specs=[hbm] * 9,
            out_specs=(inner, inner),
            scratch_shapes=[
                vmem(wide, f32), vmem(TILE, i32), vmem((6, ROWS * BLOCK), i32), vmem((6, ROWS * BLOCK), f32),
                vmem(TILE, f32), vmem(TILE, f32), small((1, 2, 4), i32), small((LEV,), f32), small((LEV,), f32),
                vmem((4, 2, LEV, BLOCK), f32), vmem((4, 2, LEV, BLOCK), f32),
                                vmem((4, ROWS + 12, BLOCK), i32), vmem((4, ROWS + 12, BLOCK), i32), vmem((4, 14, BLOCK), f32), vmem((4, 14, BLOCK), f32),
                vmem((6, *TILE), i32), vmem((6, *TILE), i32), vmem((6, *TILE), f32),
                vmem((ROUNDS, 4, ROWS + 2, BLOCK), f32), vmem((ROUNDS, 4, ROWS + 2, BLOCK), f32),
                vmem((ROUNDS, 4, 2, BLOCK), f32), vmem((ROUNDS, 2, 2, 2, BLOCK), f32), vmem((ROUNDS, 2, 1, 2, BLOCK), f32),
                vmem((6, *TILE), i32), vmem((6, *TILE), i32), vmem((6, *TILE), f32), vmem((6, *TILE), f32), vmem(TILE, f32),
                dma((9,)), dma((4, 2)), dma((4, 2)), dma((4, 2)),
                dma((ROUNDS, 4, 2)), dma((ROUNDS, 4, 2)),
            ],
            compiler_params=pltpu.CompilerParams(collective_id=0, has_side_effects=True),
        )(tracer, levels, near, weight, ssh.reshape(TILE), velocity.reshape(TILE), jnp.transpose(slots, (0, 2, 1)), thickness, profile)
        tile = jax.ShapeDtypeStruct(TILE, f32)
        out = pl.pallas_call(
            finish,
            out_shape=(jax.ShapeDtypeStruct(wide, f32), tile, tile),
            in_specs=[inner] * 2,
            out_specs=(hbm, hbm, hbm),
            scratch_shapes=[vmem(wide, f32), dma((ROWS + 2,))],
        )(*(pltpu.with_memory_space_constraint(x, pltpu.VMEM) for x in (base, tail)))
        return out[0], out[1].reshape(-1), out[2].reshape(-1)

    placed = (P(None, "dom"), P("dom"), P(None, "dom"), P(None, "dom"), P("dom"), P("dom"), P("dom", None, None), P(), P())
    return jax.shard_map(shards, mesh=mesh, in_specs=placed, out_specs=(P(None, "dom"), P("dom"), P("dom")), check_vma=False)
```

```python
import functools

import jax
import jax.numpy as jnp
from jax import lax
from jax.experimental import pallas as pl
from jax.experimental.pallas import tpu as pltpu
from jax.sharding import PartitionSpec as P

BLOCK = 128
ROWS = 8
LEV = 40
GROUPS = LEV // 8
SUBSTEPS = 6
OFFSETS = (1, -1, 2, -2)
horizontal_rate = 0.5
vertical_rate = 0.5
tracer_step = 0.2
barotropic_step = 0.5
friction = 0.05


FAR = (3, -3, 4, -4)
PLACE = (0, 2, 1, 3)
FAR_ROWS = ((0, 2), (2, 4), (1, 2), (3, 4))
ROUNDS = SUBSTEPS // 2
LAND = 2 * ROWS * BLOCK
TILE = (ROWS, BLOCK)


def along(values, index, axis):
    return jnp.take_along_axis(values, index, axis=axis, mode="promise_in_bounds")


def cols(block):
    return pl.ds(block * BLOCK, BLOCK)


def spread(row):
    return jnp.broadcast_to(row, TILE)


def kernel(
    parts, tracer_hbm, bottom_hbm, near_hbm, weight_hbm, ssh_hbm, velocity_hbm, slots_hbm, thickness_hbm, profile_hbm,
    base_v, tail_v,
    tracer_v, bottom_v, near_v, weight_v, ssh_v, velocity_v, slots, thickness, profile,
    send_tracer, halo_tracer,
    send_whole, halo_whole, send_real, halo_real, outer_row, outer_lane, outer_weight,
    send_height, halo_height, send_picked, halo_three, halo_four,
    near_row, near_lane, weight_s, near_level, forcing_v,
    copy_sem, tracer_sem, whole_sem, real_sem, height_sem, far_sem,
):
    me = lax.axis_index("dom")

    def start(source, target, number):
        copy = pltpu.make_async_copy(source, target, copy_sem.at[number])
        copy.start()
        return copy

    def inside(place):
        return (place >= 0) & (place < parts)

    barrier = pltpu.get_barrier_semaphore()
    for offset in OFFSETS + FAR:
        @pl.when(inside(me + offset))
        def _(offset=offset):
            pl.semaphore_signal(barrier, inc=1, device_id=(me + offset,), device_id_type=pl.DeviceIdType.MESH)

    slots_copy = start(slots_hbm, slots, 6)
    thickness_copy = start(thickness_hbm, thickness, 7)
    profile_copy = start(profile_hbm, profile, 8)
    tracer_copy = start(tracer_hbm, tracer_v, 4)
    bottom_copy = start(bottom_hbm, bottom_v, 1)
    near_copy = start(near_hbm, near_v, 2)
    weight_copy = start(weight_hbm, weight_v, 3)
    ssh_copy = start(ssh_hbm, ssh_v, 0)
    velocity_copy = start(velocity_hbm, velocity_v, 5)

    row_id = lax.broadcasted_iota(jnp.int32, TILE, 0)
    partner_id = row_id >> 1
    level_f = row_id.astype(jnp.float32)
    zero = jnp.zeros(TILE, jnp.float32)

    for number in range(4):
        @pl.when(jnp.logical_not(inside(me - OFFSETS[number])))
        def _(number=number):
            halo_whole[number, 0:ROWS] = jnp.full(TILE, -1, jnp.int32)
            halo_whole[number, ROWS:ROWS + 12] = jnp.full((12, BLOCK), LAND, jnp.int32)
            halo_real[number] = jnp.zeros((14, BLOCK), jnp.float32)
            halo_tracer[number] = jnp.zeros((2, LEV, BLOCK), jnp.float32)
            for turn in range(ROUNDS):
                halo_height[turn, number] = jnp.zeros((ROWS + 2, BLOCK), jnp.float32)
        @pl.when(jnp.logical_not(inside(me - FAR[number])))
        def _(number=number):
            for turn in range(ROUNDS):
                if number < 2:
                    halo_three[turn, number] = jnp.zeros((2, 2, BLOCK), jnp.float32)
                else:
                    halo_four[turn, number - 2] = jnp.zeros((1, 2, BLOCK), jnp.float32)

    def remote(source, target, sems, offset):
        return pltpu.make_async_remote_copy(
            src_ref=source, dst_ref=target, send_sem=sems.at[0], recv_sem=sems.at[1],
            device_id=(me + offset,), device_id_type=pl.DeviceIdType.MESH)

    def tracer_link(n):
        return remote(send_tracer.at[n], halo_tracer.at[n], tracer_sem.at[n], OFFSETS[n])

    def whole_link(n):
        return remote(send_whole.at[n], halo_whole.at[n], whole_sem.at[n], OFFSETS[n])

    def real_link(n):
        return remote(send_real.at[n], halo_real.at[n], real_sem.at[n], OFFSETS[n])

    def height_link(turn, n):
        return remote(send_height.at[turn, n], halo_height.at[turn, n], height_sem.at[turn, n], OFFSETS[n])

    def far_link(turn, n):
        low, high = FAR_ROWS[n]
        target = halo_three.at[turn, n] if n < 2 else halo_four.at[turn, n - 2]
        return remote(send_picked.at[turn, pl.ds(low, high - low)], target, far_sem.at[turn, n], FAR[n])

    def begin(links, offsets=OFFSETS):
        for number in range(4):
            @pl.when(inside(me + offsets[number]))
            def _(number=number):
                for link in links:
                    link(number).start()

    def arrive(links, offsets=OFFSETS):
        for number in range(4):
            @pl.when(inside(me - offsets[number]))
            def _(number=number):
                for link in links:
                    link(number).wait_recv()

    def leave(links, offsets=OFFSETS):
        for number in range(4):
            @pl.when(inside(me + offsets[number]))
            def _(number=number):
                for link in links:
                    link(number).wait_send()

    slots_copy.wait()
    chosen = zero.astype(jnp.int32)
    for number in range(4):
        for slot in range(2):
            chosen = jnp.where(row_id == 2 * number + slot, slots[0, slot, number], chosen)
    for number in range(4):
        send_whole[number, 0:ROWS] = chosen

    def pick(values, choice):
        return jnp.where(choice >= 0, along(values, jnp.maximum(choice, 0), 0), 0.0)

    def put_round(turn, height, push):
        picked = pick(height, chosen)
        pushed = pick(push, chosen)
        for number in range(4):
            send_picked[turn, PLACE[number]] = picked[2 * number:2 * number + 2]
            send_height[turn, number, 0:ROWS] = height
            send_height[turn, number, ROWS:ROWS + 2] = pushed[2 * number:2 * number + 2]
        return picked

    bottom_copy.wait()
    levels = bottom_v[...].astype(jnp.float32)
    sent_levels = pick(levels, chosen)
    for number in range(4):
        send_real[number, 12:14] = sent_levels[2 * number:2 * number + 2]
    thickness_copy.wait()
    profile_copy.wait()
    thick = []
    for group in range(GROUPS):
        t, p = zero, zero
        for k in range(8):
            t = jnp.where(row_id == k, thickness[group * 8 + k], t)
            p = jnp.where(row_id == k, profile[group * 8 + k], p)
        thick.append(t)
        tail_v[4 + group] = p
    tail_v[3] = levels
    tracer_copy.wait()
    for block in range(ROWS):
        own = spread(levels[block:block + 1])
        top, under = zero, zero
        for group in range(GROUPS):
            layer = jnp.where(level_f + float(group * 8) < own, thick[group], 0.0)
            top = top + layer * tracer_v[pl.ds(group * 8, 8), cols(block)]
            under = under + layer
        forcing_v[block:block + 1] = jnp.sum(top, axis=0, keepdims=True) / jnp.sum(under, axis=0, keepdims=True)
    forcing = forcing_v[...]
    ssh_copy.wait()
    velocity_copy.wait()
    height = ssh_v[...]

    def pushed_by(speed):
        return (1.0 - friction) * speed + barotropic_step * forcing

    push = pushed_by(velocity_v[...])
    picked = put_round(0, height, push)

    near_copy.wait()
    weight_copy.wait()
    total_weight = zero
    for column in range(6):
        for block in range(ROWS):
            near_row[column, block:block + 1] = near_v[column:column + 1, cols(block)]
            weight_s[column, block:block + 1] = weight_v[column:column + 1, cols(block)]
    for column in range(6):
        index = near_row[column]
        weight = weight_s[column]
        total_weight = total_weight + weight
        sent_index = along(index, jnp.maximum(chosen, 0), 0)
        sent_weight = pick(weight, chosen)
        for number in range(4):
            send_whole[number, ROWS + 2 * column:ROWS + 2 * column + 2] = sent_index[2 * number:2 * number + 2]
            send_real[number, 2 * column:2 * column + 2] = sent_weight[2 * number:2 * number + 2]
        near_lane[column] = index & (BLOCK - 1)
        near_row[column] = index >> 7
    for place in range(ROWS):
        which = spread(chosen[place:place + 1])
        for group in range(GROUPS):
            piece = zero
            for block in range(ROWS):
                piece = jnp.where(which == block, tracer_v[pl.ds(group * 8, 8), cols(block)], piece)
            send_tracer[place // 2, place % 2, pl.ds(group * 8, 8), :] = piece

    pl.semaphore_wait(barrier, sum(inside(me + offset).astype(jnp.int32) for offset in OFFSETS + FAR))
    begin([functools.partial(height_link, 0)])
    begin([functools.partial(far_link, 0)], FAR)
    begin([whole_link, real_link])
    begin([tracer_link])

    def gather(rows, first_row, columns, sums):
        sums = list(sums)
        count = rows.shape[0]
        wide = [spread(rows[r:r + 1]) for r in range(count)]
        for i, (row, lane) in enumerate(columns):
            for r in range(count):
                sums[i] = jnp.where(row == first_row + r, along(wide[r], lane, 1), sums[i])
        return sums

    def own_columns():
        return [(near_row[column], near_lane[column]) for column in range(6)]

    def own_update(sums, height, push):
        laplace = -total_weight * height
        for column in range(6):
            laplace = laplace + weight_s[column] * sums[column]
        speed = push + barotropic_step * laplace
        return speed, height + barotropic_step * speed

    def tracer_block(block, carry):
        at = pl.ds(pl.multiple_of(block * BLOCK, BLOCK), BLOCK)
        fields = [tracer_v[pl.ds(group * 8, 8), at] for group in range(GROUPS)]
        own = spread(bottom_v[pl.ds(block, 1), :].astype(jnp.float32))
        sums = [zero] * GROUPS
        for column in range(6):
            index = spread(near_v[column:column + 1, at])
            weight = spread(weight_v[column:column + 1, at])
            depth = spread(near_level[column, pl.ds(block, 1), :])
            lane = index & (BLOCK - 1)
            row = index >> 7
            got = [zero] * GROUPS
            for r in range(2 * ROWS):
                here = row == r
                for group in range(GROUPS):
                    if r < ROWS:
                        table = tracer_v[pl.ds(group * 8, 8), cols(r)]
                    else:
                        table = halo_tracer[(r - ROWS) // 2, (r - ROWS) % 2, pl.ds(group * 8, 8), :]
                    got[group] = jnp.where(here, along(table, lane, 1), got[group])
            for group in range(GROUPS):
                wet = jnp.where(level_f + float(group * 8) < depth, weight, 0.0)
                sums[group] = sums[group] + wet * (got[group] - fields[group])
        for group in range(GROUPS):
            here = fields[group]
            k = level_f + float(group * 8)
            down = jnp.concatenate([here[1:], fields[group + 1][:1] if group < GROUPS - 1 else here[7:]], axis=0)
            up = jnp.concatenate([fields[group - 1][7:] if group else here[:1], here[:7]], axis=0)
            vertical = jnp.where(k + 1.0 < own, down - here, 0.0) + (up - here)
            tendency = horizontal_rate * sums[group] + vertical_rate * vertical
            base_v[pl.ds(group * 8, 8), at] = here + jnp.where(k < own, tracer_step * tendency, 0.0)
        return carry

    summed = zero
    for turn in range(ROUNDS):
        if turn == 1:
            arrive([tracer_link])
        if turn >= 1:
            lax.fori_loop(4 * (turn - 1), 4 * turn, tracer_block, 0)
        sums = gather(height, 0, own_columns(), [zero] * 6)
        if turn == ROUNDS - 1:
            leave([whole_link, real_link, tracer_link])
            for earlier in range(ROUNDS):
                leave([functools.partial(far_link, earlier)], FAR)
                leave([functools.partial(height_link, earlier)])
        arrive([functools.partial(height_link, turn)] + ([whole_link, real_link] if turn == 0 else []))
        if turn == 0:
            for column in range(6):
                index = jnp.concatenate([halo_whole[n, ROWS + 2 * column:ROWS + 2 * column + 2] for n in range(4)], axis=0)
                outer_lane[column] = index & (BLOCK - 1)
                outer_row[column] = index >> 7
                outer_weight[column] = jnp.concatenate([halo_real[n, 2 * column:2 * column + 2] for n in range(4)], axis=0)
        fields = [halo_height[turn, n, 0:ROWS] for n in range(4)]
        choices = [halo_whole[n, 0:ROWS] for n in range(4)]
        picks = [pick(fields[n], choices[n]) for n in range(4)]
        halo = jnp.concatenate([picks[n][2 * n:2 * n + 2] for n in range(4)], axis=0)
        alive = jnp.concatenate([choices[n][2 * n:2 * n + 2] for n in range(4)], axis=0)
        sums = gather(halo, ROWS, own_columns(), sums)

        def mixed(rows):
            tile = zero
            for h in range(4):
                if rows[h] is not None:
                    tile = jnp.where(partner_id == h, spread(rows[h]), tile)
            return tile

        def outer_gather(tiles):
            found = [zero] * 6
            for column in range(6):
                row = outer_row[column]
                lane = outer_lane[column]
                for r, tile in tiles:
                    found[column] = jnp.where(row == r, along(tile, lane, 1), found[column])
            total = zero
            for column in range(6):
                total = total + outer_weight[column] * found[column]
            return total

        tiles = [(r, mixed([fields[h][r:r + 1] for h in range(4)])) for r in range(ROWS)]
        def close_row(h, g, slot):
            gap, at = OFFSETS[h] + OFFSETS[g], 2 * g + slot
            if gap == 0:
                return picked[at:at + 1]
            return picks[OFFSETS.index(gap)][at:at + 1] if gap in OFFSETS else None

        apart = 2 * (partner_id & 1)
        for slot in range(2):
            tiles.append((ROWS + slot, mixed([close_row(h, 0, slot) for h in range(4)])))
            tiles.append((ROWS + 2 + slot, mixed([close_row(h, 1, slot) for h in range(4)])))
            tiles.append((ROWS + 6 + slot - apart, mixed([close_row(h, 3 - h % 2, slot) for h in range(4)])))
        outer = jnp.concatenate([halo_height[turn, n, ROWS:ROWS + 2] for n in range(4)], axis=0)
        weight = zero
        for column in range(6):
            weight = weight + outer_weight[column]
        outer = outer + barotropic_step * (outer_gather(tiles) - weight * halo)
        speed, height = own_update(sums, height, push)
        push = pushed_by(speed)
        summed = summed + speed
        sums = gather(height, 0, own_columns(), [zero] * 6)

        arrive([functools.partial(far_link, turn)], FAR)
        tiles = []
        for first in (0, 2):
            for slot in range(2):
                rows = []
                for h in range(4):
                    g = first + h % 2
                    gap = OFFSETS[h] + OFFSETS[g]
                    if gap in FAR:
                        f = FAR.index(gap)
                        at = PLACE[g] - FAR_ROWS[f][0]
                        rows.append((halo_three[turn, f, at] if f < 2 else halo_four[turn, f - 2, at])[slot:slot + 1])
                    else:
                        rows.append(None)
                tiles.append((ROWS + 2 * first + slot + apart, mixed(rows)))
        outer = outer + barotropic_step * outer_gather(tiles)
        halo = jnp.where(alive >= 0, halo + barotropic_step * outer, 0.0)
        sums = gather(halo, ROWS, own_columns(), sums)
        speed, height = own_update(sums, height, push)
        push = pushed_by(speed)
        summed = summed + speed
        if turn < ROUNDS - 1:
            picked = put_round(turn + 1, height, push)
            begin([functools.partial(height_link, turn + 1)])
            begin([functools.partial(far_link, turn + 1)], FAR)
        if turn == 0:
            depths = gather(levels, 0, own_columns(), [zero] * 6)
            around = jnp.concatenate([halo_real[n, 12:14] for n in range(4)], axis=0)
            depths = gather(around, ROWS, own_columns(), depths)
            for column in range(6):
                near_level[column] = depths[column]

    tail_v[0] = height
    tail_v[1] = speed
    tail_v[2] = summed * (1.0 / SUBSTEPS)


def finish(base_v, tail_v, tracer_out, ssh_out, velocity_out, result_v, out_sem):
    height_back = pltpu.make_async_copy(tail_v.at[0], ssh_out, out_sem.at[ROWS])
    speed_back = pltpu.make_async_copy(tail_v.at[1], velocity_out, out_sem.at[ROWS + 1])
    height_back.start()
    speed_back.start()
    mean = tail_v[2]
    levels = tail_v[3]
    level_f = lax.broadcasted_iota(jnp.int32, TILE, 0).astype(jnp.float32)
    shape = [tail_v[4 + group] for group in range(GROUPS)]
    backs = []
    for block in range(ROWS):
        own = spread(levels[block:block + 1])
        push = spread(mean[block:block + 1])
        for group in range(GROUPS):
            at = (pl.ds(group * 8, 8), cols(block))
            result_v[at] = base_v[at] + jnp.where(level_f + float(group * 8) < own, shape[group] * push, 0.0)
        if block % 4 == 3:
            half = pl.ds((block - 3) * BLOCK, 4 * BLOCK)
            backs.append(pltpu.make_async_copy(result_v.at[:, half], tracer_out.at[:, half], out_sem.at[block]))
            backs[-1].start()
    height_back.wait()
    speed_back.wait()
    for back in backs:
        back.wait()


def solution(mesh):
    parts = mesh.shape["dom"]

    def shards(tracer, bottom, near, weight, ssh, velocity, slots, thickness, profile):
        hbm = pl.BlockSpec(memory_space=pltpu.HBM)
        inner = pl.BlockSpec(memory_space=pltpu.VMEM)
        f32, i32 = jnp.float32, jnp.int32
        wide = (LEV, ROWS * BLOCK)
        dma = pltpu.SemaphoreType.DMA
        vmem, small = pltpu.VMEM, pltpu.SMEM
        levels = bottom.reshape(TILE)
        base, tail = pl.pallas_call(
            functools.partial(kernel, parts),
            out_shape=(vmem(wide, f32), vmem((4 + GROUPS, *TILE), f32)),
            in_specs=[hbm] * 9,
            out_specs=(inner, inner),
            scratch_shapes=[
                vmem(wide, f32), vmem(TILE, i32), vmem((6, ROWS * BLOCK), i32), vmem((6, ROWS * BLOCK), f32),
                vmem(TILE, f32), vmem(TILE, f32), small((1, 2, 4), i32), small((LEV,), f32), small((LEV,), f32),
                vmem((4, 2, LEV, BLOCK), f32), vmem((4, 2, LEV, BLOCK), f32),
                                vmem((4, ROWS + 12, BLOCK), i32), vmem((4, ROWS + 12, BLOCK), i32), vmem((4, 14, BLOCK), f32), vmem((4, 14, BLOCK), f32),
                vmem((6, *TILE), i32), vmem((6, *TILE), i32), vmem((6, *TILE), f32),
                vmem((ROUNDS, 4, ROWS + 2, BLOCK), f32), vmem((ROUNDS, 4, ROWS + 2, BLOCK), f32),
                vmem((ROUNDS, 4, 2, BLOCK), f32), vmem((ROUNDS, 2, 2, 2, BLOCK), f32), vmem((ROUNDS, 2, 1, 2, BLOCK), f32),
                vmem((6, *TILE), i32), vmem((6, *TILE), i32), vmem((6, *TILE), f32), vmem((6, *TILE), f32), vmem(TILE, f32),
                dma((9,)), dma((4, 2)), dma((4, 2)), dma((4, 2)),
                dma((ROUNDS, 4, 2)), dma((ROUNDS, 4, 2)),
            ],
            compiler_params=pltpu.CompilerParams(collective_id=0, has_side_effects=True),
        )(tracer, levels, near, weight, ssh.reshape(TILE), velocity.reshape(TILE), jnp.transpose(slots, (0, 2, 1)), thickness, profile)
        tile = jax.ShapeDtypeStruct(TILE, f32)
        out = pl.pallas_call(
            finish,
            out_shape=(jax.ShapeDtypeStruct(wide, f32), tile, tile),
            in_specs=[inner] * 2,
            out_specs=(hbm, hbm, hbm),
            scratch_shapes=[vmem(wide, f32), dma((ROWS + 2,))],
        )(*(pltpu.with_memory_space_constraint(x, pltpu.VMEM) for x in (base, tail)))
        return out[0], out[1].reshape(-1), out[2].reshape(-1)

    placed = (P(None, "dom"), P("dom"), P(None, "dom"), P(None, "dom"), P("dom"), P("dom"), P("dom", None, None), P(), P())
    return jax.shard_map(shards, mesh=mesh, in_specs=placed, out_specs=(P(None, "dom"), P("dom"), P("dom")), check_vma=False)
```
